8 devices in a mesh: dp: 1 (over z), col: 2 (over y), row: 4 (over x, core).
Axes of the slice: x: 2, y: 2, z: 1, core: 2. Of those that a mesh axis runs over, the one named last changes fastest.
Arguments:
- x_in: bfloat16 [2, 4096, 1024], P(None, ('dp', 'row'), 'col')
- ln_gamma: float32 [1024], P('col')
- w_in: bfloat16 [1024, 4096], P('row', 'col')
- w_out: bfloat16 [4096, 1024], P('row', 'col')
Outputs:
- output: bfloat16 [2, 4096, 1024], P(None, ('dp', 'row'), 'col')
All inputs are finite; a program needn't handle non-finite values.
Results may differ from the reference program's by a relative error of at most 0.001.
Values are sent between devices in bfloat16 or wider.
A program may use at most 1 GiB of HBM per device.

```python
import jax
import jax.numpy as jnp
from jax import lax

D_MODEL = 1024
D_FF = 4096
MB_TOKENS = 4096
ROW_BLOCK = 1024
LN_EPS = 1e-5
N_BLOCKS = 2 * MB_TOKENS // ROW_BLOCK


def setup_inputs(seed: int = 0, part: int = 0) -> dict:
    base_key = jax.random.key(seed)
    part_key = jax.random.fold_in(base_key, part)
    key_noise, key_off, key_tilt, key_col = jax.random.split(part_key, 4)
    shared_key = jax.random.key(seed + 1)
    key_gamma, key_win, key_wout = jax.random.split(shared_key, 3)
    ramp = jnp.arange(D_MODEL, dtype=jnp.float32) / D_MODEL
    col_scale = (0.4 + 1.2 * ramp) * jax.random.uniform(key_col, (D_MODEL,), jnp.float32, 0.8, 1.2)
    noise = jax.random.normal(key_noise, (2, MB_TOKENS, D_MODEL), jnp.float32)
    row_off = 0.5 * jax.random.normal(key_off, (2, MB_TOKENS, 1), jnp.float32)
    row_tilt = jax.random.normal(key_tilt, (2, MB_TOKENS, 1), jnp.float32)
    x_val = row_off + row_tilt * (ramp - 0.5) + col_scale * noise
    ln_gamma = jax.random.uniform(key_gamma, (D_MODEL,), jnp.float32, 0.5, 1.5)
    w_in = jax.random.normal(key_win, (D_MODEL, D_FF), jnp.float32) * D_MODEL ** -0.5
    w_out = jax.random.normal(key_wout, (D_FF, D_MODEL), jnp.float32) * (1.5 * D_FF ** -0.5)
    return {"x_in": x_val.astype(jnp.bfloat16), "ln_gamma": ln_gamma, "w_in": w_in.astype(jnp.bfloat16), "w_out": w_out.astype(jnp.bfloat16)}


def reference(x_in, ln_gamma, w_in, w_out):
    row_blocks = x_in.reshape(N_BLOCKS, ROW_BLOCK, D_MODEL)

    def one_block(x_blk):
        x_f32 = x_blk.astype(jnp.float32)
        row_mean = jnp.sum(x_f32, axis=-1, keepdims=True) / D_MODEL
        row_var = jnp.sum(x_f32 * x_f32, axis=-1, keepdims=True) / D_MODEL - row_mean * row_mean
        z_norm = ((x_f32 - row_mean) * lax.rsqrt(row_var + LN_EPS) * ln_gamma).astype(jnp.bfloat16)
        hidden = jnp.dot(z_norm, w_in, preferred_element_type=jnp.float32)
        hidden = jax.nn.gelu(hidden, approximate=True).astype(jnp.bfloat16)
        branch = jnp.dot(hidden, w_out, preferred_element_type=jnp.float32)
        return (x_f32 + branch).astype(jnp.bfloat16)

    return lax.map(one_block, row_blocks).reshape(2, MB_TOKENS, D_MODEL)
```

```python
import functools

import jax
import jax.numpy as jnp
from jax import lax
from jax.experimental import pallas as pl
from jax.experimental.pallas import tpu as pltpu
from jax.sharding import PartitionSpec as P

LN_EPS = 1e-5
MESH = pl.DeviceIdType.MESH
TC = 256
PC = 256
SQRT_2_OVER_PI = 0.7978845608028654

KINDS = dict(w1x=8, w1y=8, w1d=8, w1xd=8, w1yx=8, w1yd=8, w1dd=8, w2x=4, w2d=4, w2xd=4, x=8, g=1)
BASE = {}
_n = 0
for _k, _c in KINDS.items():
    BASE[_k] = _n
    _n += _c
N_COPIES = _n


def gelu(u):
    inner = u * (SQRT_2_OVER_PI + (SQRT_2_OVER_PI * 0.044715) * (u * u))
    return ((0.5 * u) * (1.0 + jnp.tanh(inner))).astype(jnp.bfloat16)


def kernel(x_hbm, g_hbm, w1_hbm, w2_hbm, y_hbm, xs, gs, w1s, w2s, zs, acc, ys, load_sem, out_sem, send_sem, recv_sem):
    n_chunks = xs.shape[1]
    n_w2 = w2_hbm.shape[0] // PC
    rows1 = w1_hbm.shape[0]
    d_model = zs.shape[2]
    half_d = d_model // 2

    col = lax.axis_index("col")
    row = lax.axis_index("row")
    row_p = row + 1 - 2 * (row % 2)
    row_x = (row + 2) % 4
    row_xp = (row_p + 2) % 4
    other = 1 - col
    partner, x_nbr, y_nbr = {"row": row_p}, {"row": row_x}, {"col": other}

    def piece(half, e):
        return half * 8 + (e % 2) * 4 + e // 2

    def blk(half, e, r):
        return w1s.at[piece(half, e), pl.ds(pl.multiple_of(r * rows1, rows1), rows1)]

    def w2p(r, j):
        return w2s.at[r * n_w2 + j]

    table = dict(
        w1x=(x_nbr, lambda e: blk(col, e, row), lambda e: blk(col, e, row_x)),
        w1y=(y_nbr, lambda e: blk(col, e, row), lambda e: blk(other, e, row)),
        w1d=(partner, lambda e: blk(col, e, row), lambda e: blk(col, e, row_p)),
        w1xd=(partner, lambda e: blk(col, e, row_x), lambda e: blk(col, e, row_xp)),
        w1yx=(x_nbr, lambda e: blk(other, e, row), lambda e: blk(other, e, row_x)),
        w1yd=(partner, lambda e: blk(other, e, row), lambda e: blk(other, e, row_p)),
        w1dd=(partner, lambda e: blk(other, e, row_x), lambda e: blk(other, e, row_xp)),
        w2x=(x_nbr, lambda j: w2p(row, j), lambda j: w2p(row_x, j)),
        w2d=(partner, lambda j: w2p(row, j), lambda j: w2p(row_p, j)),
        w2xd=(partner, lambda j: w2p(row_x, j), lambda j: w2p(row_xp, j)),
        x=(y_nbr, lambda i: xs.at[col, i], lambda i: xs.at[other, i]),
        g=(y_nbr, lambda i: gs.at[col], lambda i: gs.at[other]),
    )

    def copy(kind, i, ref):
        k = BASE[kind] + i
        return pltpu.make_async_remote_copy(
            src_ref=ref, dst_ref=ref, send_sem=send_sem.at[k], recv_sem=recv_sem.at[k],
            device_id=table[kind][0], device_id_type=MESH)

    def send(kind, i):
        copy(kind, i, table[kind][1](i)).start()

    def arrive(kind, i):
        copy(kind, i, table[kind][2](i)).wait_recv()

    loads = {}

    def load(key, src, dst):
        loads[key] = pltpu.make_async_copy(src, dst, load_sem.at[len(loads)])
        loads[key].start()

    def load_w1(e):
        cols = pl.ds(pl.multiple_of((e % 2) * (4 * PC) + (e // 2) * PC, PC), PC)
        load(("w1", e), w1_hbm.at[:, cols], blk(col, e, row))

    load("g", g_hbm, gs.at[col])
    for s in range(4):
        load_w1(2 * s)
        load_w1(2 * s + 1)
        load(("w2", s), w2_hbm.at[pl.ds(s * PC, PC)], w2p(row, s))
        for i in (2 * s, 2 * s + 1):
            load(("x", i), x_hbm.at[i], xs.at[col, i])

    barrier = pltpu.get_barrier_semaphore()
    for dev in (partner, x_nbr, y_nbr):
        pl.semaphore_signal(barrier, inc=1, device_id=dev, device_id_type=MESH)
    pl.semaphore_wait(barrier, 3)

    loads["g"].wait()
    send("g", 0)

    def issue(s):
        for e in (2 * s, 2 * s + 1):
            loads[("w1", e)].wait()
            send("w1x", e)
            send("w1d", e)
        loads[("w2", s)].wait()
        send("w2x", s)
        send("w2d", s)
        for i in (2 * s, 2 * s + 1):
            loads[("x", i)].wait()
            send("x", i)

    def layer_norm(i):
        rb = 64

        def step(t, _):
            rows = pl.ds(pl.multiple_of(t * rb, rb), rb)
            parts = [xs[h, i, rows, :].astype(jnp.float32) for h in range(2)]
            mean = sum(jnp.sum(v, axis=-1, keepdims=True) for v in parts) / d_model
            var = sum(jnp.sum(v * v, axis=-1, keepdims=True) for v in parts) / d_model - mean * mean
            inv = lax.rsqrt(var + LN_EPS)
            for h in range(2):
                zs[i, rows, h * half_d:(h + 1) * half_d] = ((parts[h] - mean) * inv * gs[h]).astype(jnp.bfloat16)
            acc[i, rows, :] = xs[col, i, rows, :].astype(jnp.float32)
            return 0

        lax.fori_loop(0, TC // rb, step, 0)

    def tile(c, pieces):
        z = zs[c]
        out = None
        for p in pieces:
            h = gelu(jnp.dot(z, w1s[p], preferred_element_type=jnp.float32))
            term = jnp.dot(h, w2s[p], preferred_element_type=jnp.float32)
            out = term if out is None else out + term
        acc[c] += out

    def pair(half, j):
        return piece(half, 2 * j), piece(half, 2 * j + 1)

    def run(lo, hi, f):
        lax.fori_loop(lo, hi, lambda t, _: (f(t), 0)[1], 0)

    issue(0)
    issue(1)
    arrive("g", 0)
    for s in range(4):
        if s + 2 < 4:
            issue(s + 2)
        if s == 2:
            for e in range(8):
                send("w1y", e)
        for e in (2 * s, 2 * s + 1):
            arrive("w1x", e)
            send("w1xd", e)
        arrive("w2x", s)
        send("w2xd", s)
        for i in (2 * s, 2 * s + 1):
            arrive("x", i)
            layer_norm(i)
        for e in (2 * s, 2 * s + 1):
            arrive("w1d", e)
            arrive("w1xd", e)
        arrive("w2d", s)
        arrive("w2xd", s)
        run(0, 2 * s + 2, lambda c: tile(c, pair(col, s)))
        if s > 0:
            run(0, 2 * s, lambda t: tile(2 * s + t % 2, pair(col, t // 2)))

    def forward(e):
        arrive("w1y", e)
        send("w1yx", e)
        send("w1yd", e)

    forward(0)
    forward(1)
    for e in range(8):
        if e + 2 < 8:
            forward(e + 2)
        arrive("w1yx", e)
        send("w1dd", e)
        arrive("w1yd", e)
        arrive("w1dd", e)
        p = piece(other, e)
        if e < 7:
            run(0, n_chunks, lambda c: tile(c, (p,)))
        else:
            def last(c):
                tile(c, (p,))
                ys[c] = acc[c].astype(jnp.bfloat16)
                pltpu.make_async_copy(ys.at[c], y_hbm.at[c], out_sem.at[c]).start()

            run(0, n_chunks, last)

    for kind, count in KINDS.items():
        for i in range(count):
            copy(kind, i, table[kind][1](i)).wait_send()
    for c in range(n_chunks):
        pltpu.make_async_copy(ys.at[c], y_hbm.at[c], out_sem.at[c]).wait()


def solution(mesh):
    act_spec = P(None, ("dp", "row"), "col")

    def per_device(x_blk, gamma_blk, w_in_blk, w_out_blk):
        batch, tokens, feats = x_blk.shape
        rows1, cols1 = w_in_blk.shape
        n_chunks = batch * tokens // TC
        d_model = 2 * feats
        n_pieces = 2 * cols1 // PC
        n_loads = 1 + cols1 // PC + w_out_blk.shape[0] // PC + n_chunks
        y = pl.pallas_call(
            kernel,
            name="mlp",
            out_shape=jax.ShapeDtypeStruct((n_chunks, TC, feats), jnp.bfloat16),
            in_specs=[pl.BlockSpec(memory_space=pl.ANY)] * 4,
            out_specs=pl.BlockSpec(memory_space=pl.ANY),
            scratch_shapes=[
                pltpu.VMEM((2, n_chunks, TC, feats), jnp.bfloat16),
                pltpu.VMEM((2, 1, feats), jnp.float32),
                pltpu.VMEM((n_pieces, d_model, PC), jnp.bfloat16),
                pltpu.VMEM((n_pieces, PC, feats), jnp.bfloat16),
                pltpu.VMEM((n_chunks, TC, d_model), jnp.bfloat16),
                pltpu.VMEM((n_chunks, TC, feats), jnp.float32),
                pltpu.VMEM((n_chunks, TC, feats), jnp.bfloat16),
                pltpu.SemaphoreType.DMA((n_loads,)),
                pltpu.SemaphoreType.DMA((n_chunks,)),
                pltpu.SemaphoreType.DMA((N_COPIES,)),
                pltpu.SemaphoreType.DMA((N_COPIES,)),
            ],
            compiler_params=pltpu.CompilerParams(collective_id=0, has_side_effects=True, vmem_limit_bytes=48 * 1024 * 1024),
        )(x_blk.reshape(n_chunks, TC, feats), gamma_blk.reshape(1, feats), w_in_blk, w_out_blk)
        return y.reshape(x_blk.shape)

    return jax.shard_map(per_device, mesh=mesh, in_specs=(act_spec, P("col"), P("row", "col"), P("row", "col")), out_specs=act_spec, check_vma=False)
```

```python
import functools

import jax
import jax.numpy as jnp
from jax import lax
from jax.experimental import pallas as pl
from jax.experimental.pallas import tpu as pltpu
from jax.sharding import PartitionSpec as P

LN_EPS = 1e-5
MESH = pl.DeviceIdType.MESH
TC = 256
PC = 256
SQRT_2_OVER_PI = 0.7978845608028654

KINDS = dict(w1x=8, w1y=8, w1d=8, w1xd=8, w1yx=8, w1yd=8, w1dd=8, w2x=4, w2d=4, w2xd=4, x=8, g=1)
BASE = {}
_n = 0
for _k, _c in KINDS.items():
    BASE[_k] = _n
    _n += _c
N_COPIES = _n


def gelu(u):
    inner = u * (SQRT_2_OVER_PI + (SQRT_2_OVER_PI * 0.044715) * (u * u))
    return ((0.5 * u) * (1.0 + jnp.tanh(inner))).astype(jnp.bfloat16)


def kernel(x_hbm, g_hbm, w1_hbm, w2_hbm, ys, xs, gs, w1s, w2s, zs, acc, load_sem, send_sem, recv_sem):
    n_chunks = xs.shape[1]
    n_w2 = w2_hbm.shape[0] // PC
    rows1 = w1_hbm.shape[0]
    d_model = zs.shape[2]
    half_d = d_model // 2

    col = lax.axis_index("col")
    row = lax.axis_index("row")
    row_p = row + 1 - 2 * (row % 2)
    row_x = (row + 2) % 4
    row_xp = (row_p + 2) % 4
    other = 1 - col
    partner, x_nbr, y_nbr = {"row": row_p}, {"row": row_x}, {"col": other}

    def piece(half, e):
        return half * 8 + (e % 2) * 4 + e // 2

    def blk(half, e, r):
        return w1s.at[piece(half, e), pl.ds(pl.multiple_of(r * rows1, rows1), rows1)]

    def w2p(r, j):
        return w2s.at[r * n_w2 + j]

    table = dict(
        w1x=(x_nbr, lambda e: blk(col, e, row), lambda e: blk(col, e, row_x)),
        w1y=(y_nbr, lambda e: blk(col, e, row), lambda e: blk(other, e, row)),
        w1d=(partner, lambda e: blk(col, e, row), lambda e: blk(col, e, row_p)),
        w1xd=(partner, lambda e: blk(col, e, row_x), lambda e: blk(col, e, row_xp)),
        w1yx=(x_nbr, lambda e: blk(other, e, row), lambda e: blk(other, e, row_x)),
        w1yd=(partner, lambda e: blk(other, e, row), lambda e: blk(other, e, row_p)),
        w1dd=(partner, lambda e: blk(other, e, row_x), lambda e: blk(other, e, row_xp)),
        w2x=(x_nbr, lambda j: w2p(row, j), lambda j: w2p(row_x, j)),
        w2d=(partner, lambda j: w2p(row, j), lambda j: w2p(row_p, j)),
        w2xd=(partner, lambda j: w2p(row_x, j), lambda j: w2p(row_xp, j)),
        x=(y_nbr, lambda i: xs.at[col, i], lambda i: xs.at[other, i]),
        g=(y_nbr, lambda i: gs.at[col], lambda i: gs.at[other]),
    )

    def copy(kind, i, ref):
        k = BASE[kind] + i
        return pltpu.make_async_remote_copy(
            src_ref=ref, dst_ref=ref, send_sem=send_sem.at[k], recv_sem=recv_sem.at[k],
            device_id=table[kind][0], device_id_type=MESH)

    def send(kind, i):
        copy(kind, i, table[kind][1](i)).start()

    def arrive(kind, i):
        copy(kind, i, table[kind][2](i)).wait_recv()

    loads = {}

    def load(key, src, dst):
        loads[key] = pltpu.make_async_copy(src, dst, load_sem.at[len(loads)])
        loads[key].start()

    def load_w1(e):
        cols = pl.ds(pl.multiple_of((e % 2) * (4 * PC) + (e // 2) * PC, PC), PC)
        load(("w1", e), w1_hbm.at[:, cols], blk(col, e, row))

    load("g", g_hbm, gs.at[col])
    for s in range(4):
        load_w1(2 * s)
        load_w1(2 * s + 1)
        load(("w2", s), w2_hbm.at[pl.ds(s * PC, PC)], w2p(row, s))
        for i in (2 * s, 2 * s + 1):
            load(("x", i), x_hbm.at[i], xs.at[col, i])

    barrier = pltpu.get_barrier_semaphore()
    for dev in (partner, x_nbr, y_nbr):
        pl.semaphore_signal(barrier, inc=1, device_id=dev, device_id_type=MESH)
    pl.semaphore_wait(barrier, 3)

    loads["g"].wait()
    send("g", 0)

    def issue(s):
        for e in (2 * s, 2 * s + 1):
            loads[("w1", e)].wait()
            send("w1x", e)
            send("w1d", e)
        loads[("w2", s)].wait()
        send("w2x", s)
        send("w2d", s)
        for i in (2 * s, 2 * s + 1):
            loads[("x", i)].wait()
            if i == n_chunks - 1:
                for e in range(8):
                    send("w1y", e)
            send("x", i)

    def layer_norm(i):
        rb = 64

        def step(t, _):
            rows = pl.ds(pl.multiple_of(t * rb, rb), rb)
            parts = [xs[h, i, rows, :].astype(jnp.float32) for h in range(2)]
            mean = sum(jnp.sum(v, axis=-1, keepdims=True) for v in parts) / d_model
            var = sum(jnp.sum(v * v, axis=-1, keepdims=True) for v in parts) / d_model - mean * mean
            inv = lax.rsqrt(var + LN_EPS)
            for h in range(2):
                zs[i, rows, h * half_d:(h + 1) * half_d] = ((parts[h] - mean) * inv * gs[h]).astype(jnp.bfloat16)
            acc[i, rows, :] = xs[col, i, rows, :].astype(jnp.float32)
            return 0

        lax.fori_loop(0, TC // rb, step, 0)

    def tile(c, pieces):
        z = zs[c]
        out = None
        for p in pieces:
            h = gelu(jnp.dot(z, w1s[p], preferred_element_type=jnp.float32))
            term = jnp.dot(h, w2s[p], preferred_element_type=jnp.float32)
            out = term if out is None else out + term
        acc[c] += out

    def pair(half, j):
        return piece(half, 2 * j), piece(half, 2 * j + 1)

    def run(lo, hi, f):
        lax.fori_loop(lo, hi, lambda t, _: (f(t), 0)[1], 0)

    def pair_tiles(chunks, half, j):
        lo, hi = chunks
        run(lo, hi, lambda c: tile(c, pair(half, j)))

    def forward(j):
        for e in (2 * j, 2 * j + 1):
            arrive("w1y", e)
            send("w1yx", e)
            send("w1yd", e)

    last = n_chunks - 1
    with jax.named_scope("issue"):
        issue(0)
        issue(1)
        arrive("g", 0)
    for s in range(4):
        with jax.named_scope(f"a_wait_x{s}"):
            if s + 2 < 4:
                issue(s + 2)
            for e in (2 * s, 2 * s + 1):
                arrive("w1x", e)
                send("w1xd", e)
            arrive("w2x", s)
            send("w2xd", s)
        new = range(2 * s, min(2 * s + 2, last))
        with jax.named_scope(f"a_wait_y{s}"):
            for i in new:
                arrive("x", i)
        with jax.named_scope(f"a_norm{s}"):
            for i in new:
                layer_norm(i)
        with jax.named_scope(f"a_wait_d{s}"):
            for e in (2 * s, 2 * s + 1):
                arrive("w1d", e)
                arrive("w1xd", e)
            arrive("w2d", s)
            arrive("w2xd", s)
        with jax.named_scope(f"a_tiles{s}"):
            pair_tiles((0, new[-1] + 1), col, s)
            if s > 0:
                run(0, s * len(new), lambda t: tile(2 * s + t % len(new), pair(col, t // len(new))))

    with jax.named_scope("b_wait_first"):
        forward(0)
    for j in range(4):
        with jax.named_scope(f"b_wait_y{j}"):
            if j < 3:
                forward(j + 1)
        with jax.named_scope(f"b_wait_x{j}"):
            for e in (2 * j, 2 * j + 1):
                arrive("w1yx", e)
                send("w1dd", e)
        with jax.named_scope(f"b_wait_d{j}"):
            for e in (2 * j, 2 * j + 1):
                arrive("w1yd", e)
                arrive("w1dd", e)
        with jax.named_scope(f"b_tiles{j}"):
            pair_tiles((0, last), other, j)

    with jax.named_scope("c_wait"):
        arrive("x", last)
    with jax.named_scope("c_norm"):
        layer_norm(last)
    with jax.named_scope("c_tiles"):
        run(0, 8, lambda t: tile(last, pair(t // 4, t % 4)))

    with jax.named_scope("out"):
        def write(c):
            ys[c] = acc[c].astype(jnp.bfloat16)

        run(0, n_chunks, write)
        for kind, count in KINDS.items():
            for i in range(count):
                copy(kind, i, table[kind][1](i)).wait_send()


def solution(mesh):
    act_spec = P(None, ("dp", "row"), "col")

    def per_device(x_blk, gamma_blk, w_in_blk, w_out_blk):
        batch, tokens, feats = x_blk.shape
        rows1, cols1 = w_in_blk.shape
        n_chunks = batch * tokens // TC
        d_model = 2 * feats
        n_pieces = 2 * cols1 // PC
        n_loads = 1 + cols1 // PC + w_out_blk.shape[0] // PC + n_chunks
        y = pl.pallas_call(
            kernel,
            name="mlp",
            out_shape=jax.ShapeDtypeStruct((n_chunks, TC, feats), jnp.bfloat16),
            in_specs=[pl.BlockSpec(memory_space=pltpu.HBM)] * 4,
            out_specs=pl.BlockSpec(memory_space=pltpu.VMEM),
            scratch_shapes=[
                pltpu.VMEM((2, n_chunks, TC, feats), jnp.bfloat16),
                pltpu.VMEM((2, 1, feats), jnp.float32),
                pltpu.VMEM((n_pieces, d_model, PC), jnp.bfloat16),
                pltpu.VMEM((n_pieces, PC, feats), jnp.bfloat16),
                pltpu.VMEM((n_chunks, TC, d_model), jnp.bfloat16),
                pltpu.VMEM((n_chunks, TC, feats), jnp.float32),
                pltpu.SemaphoreType.DMA((n_loads,)),
                pltpu.SemaphoreType.DMA((N_COPIES,)),
                pltpu.SemaphoreType.DMA((N_COPIES,)),
            ],
            compiler_params=pltpu.CompilerParams(collective_id=0, has_side_effects=True, vmem_limit_bytes=52000000),
        )(*[pltpu.with_memory_space_constraint(a, pltpu.HBM) for a in (x_blk.reshape(n_chunks, TC, feats), gamma_blk.reshape(1, feats), w_in_blk, w_out_blk)])
        return y.reshape(x_blk.shape)

    return jax.shard_map(per_device, mesh=mesh, in_specs=(act_spec, P("col"), P("row", "col"), P("row", "col")), out_specs=act_spec, check_vma=False)
```

```python
import jax
import jax.numpy as jnp
from jax import lax
from jax.experimental import pallas as pl
from jax.experimental.pallas import tpu as pltpu
from jax.sharding import PartitionSpec as P

LN_EPS = 1e-5
MESH = pl.DeviceIdType.MESH
PC = 256
SQRT_2_OVER_PI = 0.7978845608028654
X_ROWS = ((0, 512), (512, 512), (1024, 512), (1536, 384), (1920, 128))

A_ICI, A_D2D, B_Y, B_X, B_D2D, X_Y, G_Y = 0, 4, 8, 16, 24, 32, 37
N_RECV = 38
S_W1, S_W2, S_X, S_G = 0, 1, 2, 3


def gelu(u):
    inner = u * (SQRT_2_OVER_PI + (SQRT_2_OVER_PI * 0.044715) * (u * u))
    return ((0.5 * u) * (1.0 + jnp.tanh(inner))).astype(jnp.bfloat16)


def kernel(x_hbm, g_hbm, w1_hbm, w2_hbm, ys, xs, w1s, w2s, zs, acc, gs, load_sem, send_sem, recv_sem):
    rows1 = w1_hbm.shape[0]
    tokens, d_model = zs.shape
    half_d = d_model // 2

    col = lax.axis_index("col")
    row = lax.axis_index("row")
    core = row % 2
    row_p = row + 1 - 2 * core
    row_x = (row + 2) % 4
    row_xp = (row_p + 2) % 4
    other = 1 - col
    partner, x_nbr, y_nbr = {"row": row_p}, {"row": row_x}, {"col": other}

    def w1p(half, e, r, n=1):
        return w1s.at[pl.ds(half * 8 + e, n), pl.ds(pl.multiple_of(r * rows1, rows1), rows1)]

    def w2p(r, j):
        return w2s.at[(r // 2) * 8 + 2 * j + r % 2]

    def send(ref, dev, s_sem, r_sem):
        pltpu.make_async_remote_copy(
            src_ref=ref, dst_ref=ref, send_sem=send_sem.at[s_sem], recv_sem=recv_sem.at[r_sem],
            device_id=dev, device_id_type=MESH).start()

    def wait(ref, sem):
        pltpu.make_async_copy(ref, ref, sem).wait()

    def load_w(s):
        for e in (2 * s, 2 * s + 1):
            cols = pl.ds((e % 2) * (4 * PC) + (e // 2) * PC, PC)
            dst = w1s.at[col * 8 + e, pl.ds(pl.multiple_of(row * rows1, rows1), rows1)]
            pltpu.make_async_copy(w1_hbm.at[:, cols], dst, load_sem.at[s]).start()
        pltpu.make_async_copy(w2_hbm.at[pl.ds(s * PC, PC)], w2p(row, s), load_sem.at[s]).start()

    def x_part(h, i):
        r0, n = X_ROWS[i]
        return xs.at[h, pl.ds(r0, n)]

    def load_x(i):
        r0, n = X_ROWS[i]
        pltpu.make_async_copy(x_hbm.at[pl.ds(r0, n)], x_part(col, i), load_sem.at[4 + i]).start()

    pltpu.make_async_copy(g_hbm, gs.at[col], load_sem.at[9]).start()
    for s in range(4):
        load_w(s)
        load_x(s)
    load_x(4)

    barrier = pltpu.get_barrier_semaphore()
    for dev in (partner, x_nbr, y_nbr):
        pl.semaphore_signal(barrier, inc=1, device_id=dev, device_id_type=MESH)
    pl.semaphore_wait(barrier, 3)

    def send_x(i):
        wait(x_part(col, i), load_sem.at[4 + i])
        send(x_part(col, i), y_nbr, S_X, X_Y + i)

    def issue(s):
        wait(w1s.at[0], load_sem.at[s])
        w1, w2 = w1p(col, 2 * s, row, 2), w2p(row, s)
        send(w1, x_nbr, S_W1, A_ICI + s)
        send(w2, x_nbr, S_W2, A_ICI + s)
        send(w1, partner, S_W1, A_D2D + s)
        send(w2, partner, S_W2, A_D2D + s)
        send_x(s)

    def relay_a(s):
        wait(w1s.at[0], recv_sem.at[A_ICI + s])
        send(w1p(col, 2 * s, row_x, 2), partner, S_W1, A_D2D + s)
        send(w2p(row_x, s), partner, S_W2, A_D2D + s)

    def relay_by(e):
        wait(w1p(other, e, row), recv_sem.at[B_Y + e])
        send(w1p(other, e, row), x_nbr, S_W1, B_X + e)
        send(w1p(other, e, row), partner, S_W1, B_D2D + e)

    def relay_bx(e):
        wait(w1p(other, e, row_x), recv_sem.at[B_X + e])
        send(w1p(other, e, row_x), partner, S_W1, B_D2D + e)

    def layer_norm(i):
        r0, n = X_ROWS[i]
        rb = 64
        wait(x_part(other, i), recv_sem.at[X_Y + i])

        def step(t, _):
            rows = pl.ds(pl.multiple_of(r0 + t * rb, rb), rb)
            parts = [xs[h, rows, :].astype(jnp.float32) for h in range(2)]
            mean = sum(jnp.sum(v, axis=-1, keepdims=True) for v in parts) / d_model
            var = sum(jnp.sum(v * v, axis=-1, keepdims=True) for v in parts) / d_model - mean * mean
            inv = lax.rsqrt(var + LN_EPS)
            for h in range(2):
                zs[rows, h * half_d:(h + 1) * half_d] = ((parts[h] - mean) * inv * gs[h]).astype(jnp.bfloat16)
            acc[rows, :] = xs[col, rows, :].astype(jnp.float32)
            return 0

        lax.fori_loop(0, n // rb, step, 0)

    def sweep(units, store=None):
        held = None

        def finish():
            r0, n, ps, hs = held
            rows = pl.ds(r0, n)
            out = None
            for p, h in zip(ps, hs):
                term = jnp.dot(h, w2s[p], preferred_element_type=jnp.float32)
                out = term if out is None else out + term
            if store is None:
                acc[rows, :] += out
            else:
                store(rows, acc[rows, :] + out)

        for r0, n, ps in units:
            z = zs[pl.ds(r0, n), :]
            hs = [gelu(jnp.dot(z, w1s[p], preferred_element_type=jnp.float32)) for p in ps]
            if held is not None:
                finish()
            held = (r0, n, ps, hs)
        finish()

    def pieces(half, lo, hi):
        return [half * 8 + e for e in range(lo, hi)]

    with jax.named_scope("issue"):
        wait(gs.at[col], load_sem.at[9])
        send(gs.at[col], y_nbr, S_G, G_Y)
        issue(0)
        issue(1)
        wait(gs.at[other], recv_sem.at[G_Y])
    for s in range(3):
        with jax.named_scope(f"a_wait_x{s}"):
            if s < 2:
                issue(s + 2)
            if s == 1:
                for e in range(8):
                    send(w1p(col, e, row), y_nbr, S_W1, B_Y + e)
                send_x(4)
            relay_a(s)
        with jax.named_scope(f"a_norm{s}"):
            layer_norm(s)
        with jax.named_scope(f"a_wait_d{s}"):
            wait(w1s.at[pl.ds(0, 2)], recv_sem.at[A_D2D + s])
        with jax.named_scope(f"a_tiles{s}"):
            def a_tile(t, _):
                q = t // (s + 1)
                g, j = t - q * (t - s), s - q * (t - s)
                p = col * 8 + 2 * j
                sweep([(pl.multiple_of(g * 512 + k, 256), 256, (p, p + 1)) for k in (0, 256)])
                return 0

            lax.fori_loop(0, 2 * s + 1, a_tile, 0)

    early = X_ROWS[4][0]
    with jax.named_scope("a_norm3"):
        layer_norm(3)
    with jax.named_scope("a_tiles3"):
        sweep([(*X_ROWS[3], pieces(col, e, e + 2)) for e in (0, 2, 4)])
    with jax.named_scope("a_wait_y3"):
        relay_by(0)
    with jax.named_scope("a_wait_x3"):
        relay_a(3)
    with jax.named_scope("a_wait_d3"):
        wait(w1s.at[pl.ds(0, 2)], recv_sem.at[A_D2D + 3])
    with jax.named_scope("a_tiles4"):
        sweep([(r, early // 4, pieces(col, 6, 8)) for r in (0, early // 4)])
    with jax.named_scope("b_wait_y"):
        relay_by(1)
    with jax.named_scope("a_tiles5"):
        sweep([(r, early // 4, pieces(col, 6, 8)) for r in (early // 2, 3 * early // 4)])

    def b_step(e, _):
        with jax.named_scope("b_wait_x"):
            relay_bx(e)
        with jax.named_scope("b_wait_y"):
            @pl.when(e < 6)
            def _():
                relay_by(e + 2)
        with jax.named_scope("b_wait_d"):
            wait(w2s.at[0], recv_sem.at[B_D2D + e])
        with jax.named_scope("b_tile"):
            sweep([(r, early // 4, (other * 8 + e,)) for r in range(0, early, early // 4)])
        return 0

    lax.fori_loop(0, 7, b_step, 0)
    with jax.named_scope("c_relay"):
        relay_bx(7)
    with jax.named_scope("c_norm"):
        layer_norm(4)
    with jax.named_scope("c_tiles"):
        last = (pieces(col, 0, 8) + pieces(other, 0, 7))
        sweep([(early, tokens - early, last[k:k + 2]) for k in range(0, len(last), 2)])
    with jax.named_scope("d_wait"):
        wait(w2s.at[0], recv_sem.at[B_D2D + 7])
    with jax.named_scope("d_tile"):
        def write(rows, value):
            ys[rows, :] = value.astype(jnp.bfloat16)

        sweep([(r, tokens // 4, (other * 8 + 7,)) for r in range(0, tokens, tokens // 4)], write)

    with jax.named_scope("sent"):
        wait(w1s.at[pl.ds(0, 14)], send_sem.at[S_W1])
        wait(w2s.at[pl.ds(0, 12)], send_sem.at[S_W2])
        wait(xs.at[0], send_sem.at[S_X])
        wait(gs.at[0], send_sem.at[S_G])


def solution(mesh):
    act_spec = P(None, ("dp", "row"), "col")

    def per_device(x_blk, gamma_blk, w_in_blk, w_out_blk):
        feats = x_blk.shape[2]
        tokens = x_blk.shape[0] * x_blk.shape[1]
        d_model = 2 * feats
        n_pieces = 2 * w_in_blk.shape[1] // PC
        ins = (x_blk.reshape(tokens, feats), gamma_blk.reshape(1, feats), w_in_blk, w_out_blk)
        y = pl.pallas_call(
            kernel,
            name="mlp",
            out_shape=jax.ShapeDtypeStruct((tokens, feats), jnp.bfloat16),
            in_specs=[pl.BlockSpec(memory_space=pltpu.HBM)] * 4,
            out_specs=pl.BlockSpec(memory_space=pltpu.VMEM),
            scratch_shapes=[
                pltpu.VMEM((2, tokens, feats), jnp.bfloat16),
                pltpu.VMEM((n_pieces, d_model, PC), jnp.bfloat16),
                pltpu.VMEM((n_pieces, PC, feats), jnp.bfloat16),
                pltpu.VMEM((tokens, d_model), jnp.bfloat16),
                pltpu.VMEM((tokens, feats), jnp.float32),
                pltpu.VMEM((2, 1, feats), jnp.float32),
                pltpu.SemaphoreType.DMA((10,)),
                pltpu.SemaphoreType.DMA((4,)),
                pltpu.SemaphoreType.DMA((N_RECV,)),
            ],
            compiler_params=pltpu.CompilerParams(collective_id=0, has_side_effects=True, vmem_limit_bytes=52000000),
        )(*[pltpu.with_memory_space_constraint(a, pltpu.HBM) for a in ins])
        return y.reshape(x_blk.shape)

    return jax.shard_map(per_device, mesh=mesh, in_specs=(act_spec, P("col"), P("row", "col"), P("row", "col")), out_specs=act_spec, check_vma=False)
```

```python
import jax
import jax.numpy as jnp
from jax import lax
from jax.experimental import pallas as pl
from jax.experimental.pallas import tpu as pltpu
from jax.sharding import PartitionSpec as P

LN_EPS = 1e-5
MESH = pl.DeviceIdType.MESH
PC = 256
SQRT_2_OVER_PI = 0.7978845608028654
X_ROWS = ((0, 512), (512, 512), (1024, 512), (1536, 384), (1920, 128))

A_ICI, A_D2D, B_Y, B_X, B_D2D, X_Y, G_Y = 0, 4, 8, 24, 32, 40, 45
N_RECV = 46
S_W1, S_W2, S_X, S_G = 0, 1, 2, 3


def gelu(u):
    inner = u * (SQRT_2_OVER_PI + (SQRT_2_OVER_PI * 0.044715) * (u * u))
    return ((0.5 * u) * (1.0 + jnp.tanh(inner))).astype(jnp.bfloat16)


def kernel(x_hbm, g_hbm, w1_hbm, w2_hbm, ys, xs, w1s, w2s, zs, acc, gs, load_sem, send_sem, recv_sem):
    rows1 = w1_hbm.shape[0]
    tokens, d_model = zs.shape
    half_d = d_model // 2

    col = lax.axis_index("col")
    row = lax.axis_index("row")
    core = row % 2
    row_p = row + 1 - 2 * core
    row_x = (row + 2) % 4
    row_xp = (row_p + 2) % 4
    other = 1 - col
    partner, x_nbr, y_nbr = {"row": row_p}, {"row": row_x}, {"col": other}

    def w1p(half, e, r, n=1):
        return w1s.at[pl.ds(half * 8 + e, n), pl.ds(pl.multiple_of(r * rows1, rows1), rows1)]

    def w2p(r, j):
        return w2s.at[(r // 2) * 8 + 2 * j + r % 2]

    def send(ref, dev, s_sem, r_sem):
        pltpu.make_async_remote_copy(
            src_ref=ref, dst_ref=ref, send_sem=send_sem.at[s_sem], recv_sem=recv_sem.at[r_sem],
            device_id=dev, device_id_type=MESH).start()

    def wait(ref, sem):
        pltpu.make_async_copy(ref, ref, sem).wait()

    def load_w(s):
        for e in (2 * s, 2 * s + 1):
            cols = pl.ds((e % 2) * (4 * PC) + (e // 2) * PC, PC)
            dst = w1s.at[col * 8 + e, pl.ds(pl.multiple_of(row * rows1, rows1), rows1)]
            pltpu.make_async_copy(w1_hbm.at[:, cols], dst, load_sem.at[s]).start()
        pltpu.make_async_copy(w2_hbm.at[pl.ds(s * PC, PC)], w2p(row, s), load_sem.at[s]).start()

    def x_part(h, i):
        r0, n = X_ROWS[i]
        return xs.at[h, pl.ds(r0, n)]

    def load_x(i):
        r0, n = X_ROWS[i]
        pltpu.make_async_copy(x_hbm.at[pl.ds(r0, n)], x_part(col, i), load_sem.at[4 + i]).start()

    pltpu.make_async_copy(g_hbm, gs.at[col], load_sem.at[9]).start()
    for s in range(4):
        load_w(s)
        load_x(s)
    load_x(4)

    barrier = pltpu.get_barrier_semaphore()
    for dev in (partner, x_nbr, y_nbr):
        pl.semaphore_signal(barrier, inc=1, device_id=dev, device_id_type=MESH)
    pl.semaphore_wait(barrier, 3)

    def send_x(i):
        wait(x_part(col, i), load_sem.at[4 + i])
        send(x_part(col, i), y_nbr, S_X, X_Y + i)

    def issue(s):
        wait(w1s.at[0], load_sem.at[s])
        w1, w2 = w1p(col, 2 * s, row, 2), w2p(row, s)
        send(w1, x_nbr, S_W1, A_ICI + s)
        send(w2, x_nbr, S_W2, A_ICI + s)
        send(w1, partner, S_W1, A_D2D + s)
        send(w2, partner, S_W2, A_D2D + s)
        send_x(s)

    def relay_a(s):
        wait(w1s.at[0], recv_sem.at[A_ICI + s])
        send(w1p(col, 2 * s, row_x, 2), partner, S_W1, A_D2D + s)
        send(w2p(row_x, s), partner, S_W2, A_D2D + s)

    def half_piece(half, e, h):
        return w1s.at[half * 8 + e, pl.ds(pl.multiple_of(row * rows1 + h * (rows1 // 2), rows1 // 2), rows1 // 2)]

    def relay_by(e, h):
        part = half_piece(other, e, h)
        wait(part, recv_sem.at[B_Y + 2 * e + h])
        send(part, x_nbr, S_W1, B_X + e)
        send(part, partner, S_W1, B_D2D + e)

    def relay_bx(e):
        wait(w1p(other, e, row_x), recv_sem.at[B_X + e])
        send(w1p(other, e, row_x), partner, S_W1, B_D2D + e)

    def layer_norm(i):
        r0, n = X_ROWS[i]
        rb = 64
        wait(x_part(other, i), recv_sem.at[X_Y + i])

        def step(t, _):
            rows = pl.ds(pl.multiple_of(r0 + t * rb, rb), rb)
            parts = [xs[h, rows, :].astype(jnp.float32) for h in range(2)]
            mean = sum(jnp.sum(v, axis=-1, keepdims=True) for v in parts) / d_model
            var = sum(jnp.sum(v * v, axis=-1, keepdims=True) for v in parts) / d_model - mean * mean
            inv = lax.rsqrt(var + LN_EPS)
            for h in range(2):
                zs[rows, h * half_d:(h + 1) * half_d] = ((parts[h] - mean) * inv * gs[h]).astype(jnp.bfloat16)
            acc[rows, :] = xs[col, rows, :].astype(jnp.float32)
            return 0

        lax.fori_loop(0, n // rb, step, 0)

    def sweep(units, store=None):
        held = None

        def finish():
            r0, n, ps, hs = held
            rows = pl.ds(r0, n)
            out = None
            for p, h in zip(ps, hs):
                term = jnp.dot(h, w2s[p], preferred_element_type=jnp.float32)
                out = term if out is None else out + term
            if store is None:
                acc[rows, :] += out
            else:
                store(rows, acc[rows, :] + out)

        for r0, n, ps in units:
            z = zs[pl.ds(r0, n), :]
            hs = [gelu(jnp.dot(z, w1s[p], preferred_element_type=jnp.float32)) for p in ps]
            if held is not None:
                finish()
            held = (r0, n, ps, hs)
        finish()

    def pieces(half, lo, hi):
        return [half * 8 + e for e in range(lo, hi)]

    with jax.named_scope("issue"):
        wait(gs.at[col], load_sem.at[9])
        send(gs.at[col], y_nbr, S_G, G_Y)
        issue(0)
        issue(1)
        wait(gs.at[other], recv_sem.at[G_Y])
    for s in range(3):
        with jax.named_scope(f"a_wait_x{s}"):
            if s < 2:
                issue(s + 2)
            if s == 1:
                for e in range(8):
                    for h in range(2):
                        send(half_piece(col, e, h), y_nbr, S_W1, B_Y + 2 * e + h)
                send_x(4)
            relay_a(s)
        with jax.named_scope(f"a_norm{s}"):
            layer_norm(s)
        with jax.named_scope(f"a_wait_d{s}"):
            wait(w1s.at[pl.ds(0, 2)], recv_sem.at[A_D2D + s])
        with jax.named_scope(f"a_tiles{s}"):
            def a_tile(t, _):
                q = t // (s + 1)
                g, j = t - q * (t - s), s - q * (t - s)
                p = col * 8 + 2 * j
                sweep([(pl.multiple_of(g * 512 + k, 256), 256, (p, p + 1)) for k in (0, 256)])
                return 0

            lax.fori_loop(0, 2 * s + 1, a_tile, 0)

    early = X_ROWS[4][0]
    third = early // 3
    with jax.named_scope("a_norm3"):
        layer_norm(3)
    with jax.named_scope("a_tiles3"):
        sweep([(*X_ROWS[3], pieces(col, e, e + 2)) for e in (0, 2, 4)])
    def b_sweep(e, lo, hi, n=third):
        return [(r, n, (other * 8 + e,)) for r in range(lo, hi, n)]

    def b_arrived(e):
        wait(w2s.at[0], recv_sem.at[B_D2D + e])

    with jax.named_scope("s1"):
        relay_by(0, 0)
        relay_by(0, 1)
        relay_a(3)
        wait(w1s.at[pl.ds(0, 2)], recv_sem.at[A_D2D + 3])
    for q in range(3):
        with jax.named_scope(f"s{q + 2}"):
            if q == 1:
                relay_by(1, 1)
                relay_bx(0)
            else:
                relay_by(1 + q // 2, 0)
        with jax.named_scope(f"s{q + 2}_a"):
            sweep([(q * third + r, third // 2, pieces(col, 6, 8)) for r in (0, third // 2)])
    with jax.named_scope("s5"):
        relay_by(2, 1)
        relay_bx(1)
        b_arrived(0)
    with jax.named_scope("s5_b0"):
        sweep(b_sweep(0, 0, 2 * third))
    with jax.named_scope("s6"):
        relay_by(3, 0)
        b_arrived(1)
    with jax.named_scope("s6_b01"):
        sweep(b_sweep(0, 2 * third, early) + b_sweep(1, 0, third))
    with jax.named_scope("s7"):
        relay_by(3, 1)
        relay_bx(2)
    with jax.named_scope("s7_b1"):
        sweep(b_sweep(1, third, early))

    def b_step(e, _):
        with jax.named_scope("s_even"):
            relay_by(e + 2, 0)
            b_arrived(e)
        with jax.named_scope("s_even_b"):
            sweep(b_sweep(e, 0, 2 * third))
        with jax.named_scope("s_odd"):
            relay_by(e + 2, 1)
            relay_bx(e + 1)
        with jax.named_scope("s_odd_b"):
            sweep(b_sweep(e, 2 * third, early, third // 2))
        return 0

    lax.fori_loop(2, 6, b_step, 0)
    with jax.named_scope("t_wait6"):
        b_arrived(6)
    with jax.named_scope("t_b6"):
        sweep(b_sweep(6, 0, early))
    with jax.named_scope("t_wait7"):
        relay_bx(7)
    with jax.named_scope("c_norm"):
        layer_norm(4)
    with jax.named_scope("c_tiles"):
        last = (pieces(col, 0, 8) + pieces(other, 0, 7))
        sweep([(early, tokens - early, last[k:k + 2]) for k in range(0, len(last), 2)])
    with jax.named_scope("d_wait"):
        wait(w2s.at[0], recv_sem.at[B_D2D + 7])
    with jax.named_scope("d_tile"):
        def write(rows, value):
            ys[rows, :] = value.astype(jnp.bfloat16)

        sweep([(r, tokens // 4, (other * 8 + 7,)) for r in range(0, tokens, tokens // 4)], write)

    with jax.named_scope("sent"):
        wait(w1s.at[pl.ds(0, 14)], send_sem.at[S_W1])
        wait(w2s.at[pl.ds(0, 12)], send_sem.at[S_W2])
        wait(xs.at[0], send_sem.at[S_X])
        wait(gs.at[0], send_sem.at[S_G])


def solution(mesh):
    act_spec = P(None, ("dp", "row"), "col")

    def per_device(x_blk, gamma_blk, w_in_blk, w_out_blk):
        feats = x_blk.shape[2]
        tokens = x_blk.shape[0] * x_blk.shape[1]
        d_model = 2 * feats
        n_pieces = 2 * w_in_blk.shape[1] // PC
        ins = (x_blk.reshape(tokens, feats), gamma_blk.reshape(1, feats), w_in_blk, w_out_blk)
        y = pl.pallas_call(
            kernel,
            name="mlp",
            out_shape=jax.ShapeDtypeStruct((tokens, feats), jnp.bfloat16),
            in_specs=[pl.BlockSpec(memory_space=pltpu.HBM)] * 4,
            out_specs=pl.BlockSpec(memory_space=pltpu.VMEM),
            scratch_shapes=[
                pltpu.VMEM((2, tokens, feats), jnp.bfloat16),
                pltpu.VMEM((n_pieces, d_model, PC), jnp.bfloat16),
                pltpu.VMEM((n_pieces, PC, feats), jnp.bfloat16),
                pltpu.VMEM((tokens, d_model), jnp.bfloat16),
                pltpu.VMEM((tokens, feats), jnp.float32),
                pltpu.VMEM((2, 1, feats), jnp.float32),
                pltpu.SemaphoreType.DMA((10,)),
                pltpu.SemaphoreType.DMA((4,)),
                pltpu.SemaphoreType.DMA((N_RECV,)),
            ],
            compiler_params=pltpu.CompilerParams(collective_id=0, has_side_effects=True, vmem_limit_bytes=52000000),
        )(*[pltpu.with_memory_space_constraint(a, pltpu.HBM) for a in ins])
        return y.reshape(x_blk.shape)

    return jax.shard_map(per_device, mesh=mesh, in_specs=(act_spec, P("col"), P("row", "col"), P("row", "col")), out_specs=act_spec, check_vma=False)
```

```python
import jax
import jax.numpy as jnp
from jax import lax
from jax.experimental import pallas as pl
from jax.experimental.pallas import tpu as pltpu
from jax.sharding import PartitionSpec as P

LN_EPS = 1e-5
MESH = pl.DeviceIdType.MESH
PC = 256
SQRT_2_OVER_PI = 0.7978845608028654
X_ROWS = ((0, 512), (512, 512), (1024, 512), (1536, 384), (1920, 128))

A_ICI, A_D2D, B_Y, B_X, B_D2D, X_Y, G_Y = 0, 4, 8, 24, 32, 40, 45
N_RECV = 46
S_W1, S_W2, S_X, S_G = 0, 1, 2, 3


def gelu(u):
    inner = u * (SQRT_2_OVER_PI + (SQRT_2_OVER_PI * 0.044715) * (u * u))
    return ((0.5 * u) * (1.0 + jnp.tanh(inner))).astype(jnp.bfloat16)


def kernel(x_hbm, g_hbm, w1_hbm, w2_hbm, ys, xs, w1s, w2s, zs, acc, gs, load_sem, send_sem, recv_sem):
    rows1 = w1_hbm.shape[0]
    tokens, d_model = zs.shape
    half_d = d_model // 2

    col = lax.axis_index("col")
    row = lax.axis_index("row")
    core = row % 2
    row_p = row + 1 - 2 * core
    row_x = (row + 2) % 4
    row_xp = (row_p + 2) % 4
    other = 1 - col
    partner, x_nbr, y_nbr = {"row": row_p}, {"row": row_x}, {"col": other}

    def w1p(half, e, r, n=1):
        return w1s.at[pl.ds(half * 8 + e, n), pl.ds(pl.multiple_of(r * rows1, rows1), rows1)]

    def w2p(r, j):
        return w2s.at[(r // 2) * 8 + 2 * j + r % 2]

    def send(ref, dev, s_sem, r_sem):
        pltpu.make_async_remote_copy(
            src_ref=ref, dst_ref=ref, send_sem=send_sem.at[s_sem], recv_sem=recv_sem.at[r_sem],
            device_id=dev, device_id_type=MESH).start()

    def wait(ref, sem):
        pltpu.make_async_copy(ref, ref, sem).wait()

    def load_w(s):
        for e in (2 * s, 2 * s + 1):
            cols = pl.ds((e % 2) * (4 * PC) + (e // 2) * PC, PC)
            dst = w1s.at[col * 8 + e, pl.ds(pl.multiple_of(row * rows1, rows1), rows1)]
            pltpu.make_async_copy(w1_hbm.at[:, cols], dst, load_sem.at[s]).start()
        pltpu.make_async_copy(w2_hbm.at[pl.ds(s * PC, PC)], w2p(row, s), load_sem.at[s]).start()

    def x_part(h, i):
        r0, n = X_ROWS[i]
        return xs.at[h, pl.ds(r0, n)]

    def load_x(i):
        r0, n = X_ROWS[i]
        pltpu.make_async_copy(x_hbm.at[pl.ds(r0, n)], x_part(col, i), load_sem.at[4 + i]).start()

    pltpu.make_async_copy(g_hbm, gs.at[col], load_sem.at[9]).start()
    for s in range(4):
        load_w(s)
        load_x(s)
    load_x(4)

    barrier = pltpu.get_barrier_semaphore()
    for dev in (partner, x_nbr, y_nbr):
        pl.semaphore_signal(barrier, inc=1, device_id=dev, device_id_type=MESH)
    pl.semaphore_wait(barrier, 3)

    def send_x(i):
        wait(x_part(col, i), load_sem.at[4 + i])
        send(x_part(col, i), y_nbr, S_X, X_Y + i)

    def issue(s):
        wait(w1s.at[0], load_sem.at[s])
        w1, w2 = w1p(col, 2 * s, row, 2), w2p(row, s)
        send(w1, x_nbr, S_W1, A_ICI + s)
        send(w2, x_nbr, S_W2, A_ICI + s)
        send(w1, partner, S_W1, A_D2D + s)
        send(w2, partner, S_W2, A_D2D + s)
        send_x(s)

    def relay_a(s):
        wait(w1s.at[0], recv_sem.at[A_ICI + s])
        send(w1p(col, 2 * s, row_x, 2), partner, S_W1, A_D2D + s)
        send(w2p(row_x, s), partner, S_W2, A_D2D + s)

    def half_piece(half, e, h):
        return w1s.at[half * 8 + e, pl.ds(pl.multiple_of(row * rows1 + h * (rows1 // 2), rows1 // 2), rows1 // 2)]

    def relay_by(e, h):
        part = half_piece(other, e, h)
        wait(part, recv_sem.at[B_Y + 2 * e + h])
        send(part, x_nbr, S_W1, B_X + e)
        send(part, partner, S_W1, B_D2D + e)

    def relay_bx(e):
        wait(w1p(other, e, row_x), recv_sem.at[B_X + e])
        send(w1p(other, e, row_x), partner, S_W1, B_D2D + e)

    def layer_norm(i):
        r0, n = X_ROWS[i]
        rb = 64
        wait(x_part(other, i), recv_sem.at[X_Y + i])

        def step(t, _):
            rows = pl.ds(pl.multiple_of(r0 + t * rb, rb), rb)
            parts = [xs[h, rows, :].astype(jnp.float32) for h in range(2)]
            mean = sum(jnp.sum(v, axis=-1, keepdims=True) for v in parts) / d_model
            var = sum(jnp.sum(v * v, axis=-1, keepdims=True) for v in parts) / d_model - mean * mean
            inv = lax.rsqrt(var + LN_EPS)
            for h in range(2):
                zs[rows, h * half_d:(h + 1) * half_d] = ((parts[h] - mean) * inv * gs[h]).astype(jnp.bfloat16)
            acc[rows, :] = xs[col, rows, :].astype(jnp.float32)
            return 0

        lax.fori_loop(0, n // rb, step, 0)

    def sweep(units, store=None):
        held = None

        def finish():
            r0, n, ps, hs = held
            rows = pl.ds(r0, n)
            out = None
            for p, h in zip(ps, hs):
                term = jnp.dot(h, w2s[p], preferred_element_type=jnp.float32)
                out = term if out is None else out + term
            if store is None:
                acc[rows, :] += out
            else:
                store(rows, acc[rows, :] + out)

        for r0, n, ps in units:
            z = zs[pl.ds(r0, n), :]
            hs = [gelu(jnp.dot(z, w1s[p], preferred_element_type=jnp.float32)) for p in ps]
            if held is not None:
                finish()
            held = (r0, n, ps, hs)
        finish()

    def pieces(half, lo, hi):
        return [half * 8 + e for e in range(lo, hi)]

    with jax.named_scope("issue"):
        wait(gs.at[col], load_sem.at[9])
        send(gs.at[col], y_nbr, S_G, G_Y)
        issue(0)
        issue(1)
        wait(gs.at[other], recv_sem.at[G_Y])
    for s in range(3):
        with jax.named_scope(f"a_wait_x{s}"):
            if s < 2:
                issue(s + 2)
            if s == 1:
                for e in range(8):
                    for h in range(2):
                        send(half_piece(col, e, h), y_nbr, S_W1, B_Y + 2 * e + h)
                send_x(4)
            relay_a(s)
        with jax.named_scope(f"a_norm{s}"):
            layer_norm(s)
        with jax.named_scope(f"a_wait_d{s}"):
            wait(w1s.at[pl.ds(0, 2)], recv_sem.at[A_D2D + s])
        with jax.named_scope(f"a_tiles{s}"):
            def a_tile(t, _):
                q = t // (s + 1)
                g, j = t - q * (t - s), s - q * (t - s)
                p = col * 8 + 2 * j
                sweep([(pl.multiple_of(g * 512 + k, 256), 256, (p, p + 1)) for k in (0, 256)])
                return 0

            lax.fori_loop(0, 2 * s + 1, a_tile, 0)

    early = X_ROWS[4][0]
    third = early // 3
    with jax.named_scope("a_norm3"):
        layer_norm(3)
    def b_sweep(e, lo, hi, n=early // 4):
        return [(r, n, (other * 8 + e,)) for r in range(lo, hi, n)]

    def b_arrived(e):
        wait(w2s.at[0], recv_sem.at[B_D2D + e])

    with jax.named_scope("s0_a"):
        sweep([(*X_ROWS[3], pieces(col, 0, 2))])
    with jax.named_scope("s1"):
        relay_by(0, 0)
    with jax.named_scope("s1_a"):
        sweep([(*X_ROWS[3], pieces(col, e, e + 2)) for e in (2, 4)])
    with jax.named_scope("s2"):
        relay_by(0, 1)
        relay_a(3)
    with jax.named_scope("s2_d"):
        wait(w1s.at[pl.ds(0, 2)], recv_sem.at[A_D2D + 3])
    for q in range(3):
        with jax.named_scope(f"s{q + 3}_a"):
            sweep([(q * third + r, third // 2, pieces(col, 6, 8)) for r in (0, third // 2)])
        with jax.named_scope(f"s{q + 3}"):
            if q < 2:
                relay_by(1, q)
            if q == 1:
                relay_bx(0)

    def b_step(e, _):
        with jax.named_scope("s_even"):
            relay_by(e + 2, 0)
        with jax.named_scope("s_even_d"):
            b_arrived(e)
        with jax.named_scope("s_even_b"):
            sweep(b_sweep(e, 0, early // 2))
        with jax.named_scope("s_odd"):
            relay_by(e + 2, 1)
        with jax.named_scope("s_odd_x"):
            relay_bx(e + 1)
        with jax.named_scope("s_odd_b"):
            sweep(b_sweep(e, early // 2, early))
        return 0

    lax.fori_loop(0, 6, b_step, 0)
    with jax.named_scope("t_wait6"):
        b_arrived(6)
    with jax.named_scope("t_b6"):
        sweep(b_sweep(6, 0, early))
    with jax.named_scope("t_wait7"):
        relay_bx(7)
    with jax.named_scope("c_norm"):
        layer_norm(4)
    with jax.named_scope("c_tiles"):
        last = (pieces(col, 0, 8) + pieces(other, 0, 7))
        sweep([(early, tokens - early, last[k:k + 2]) for k in range(0, len(last), 2)])
    with jax.named_scope("d_wait"):
        wait(w2s.at[0], recv_sem.at[B_D2D + 7])
    with jax.named_scope("d_tile"):
        def write(rows, value):
            ys[rows, :] = value.astype(jnp.bfloat16)

        sweep([(r, tokens // 4, (other * 8 + 7,)) for r in range(0, tokens, tokens // 4)], write)

    with jax.named_scope("sent"):
        wait(w1s.at[pl.ds(0, 14)], send_sem.at[S_W1])
        wait(w2s.at[pl.ds(0, 12)], send_sem.at[S_W2])
        wait(xs.at[0], send_sem.at[S_X])
        wait(gs.at[0], send_sem.at[S_G])


def solution(mesh):
    act_spec = P(None, ("dp", "row"), "col")

    def per_device(x_blk, gamma_blk, w_in_blk, w_out_blk):
        feats = x_blk.shape[2]
        tokens = x_blk.shape[0] * x_blk.shape[1]
        d_model = 2 * feats
        n_pieces = 2 * w_in_blk.shape[1] // PC
        ins = (x_blk.reshape(tokens, feats), gamma_blk.reshape(1, feats), w_in_blk, w_out_blk)
        y = pl.pallas_call(
            kernel,
            name="mlp",
            out_shape=jax.ShapeDtypeStruct((tokens, feats), jnp.bfloat16),
            in_specs=[pl.BlockSpec(memory_space=pltpu.HBM)] * 4,
            out_specs=pl.BlockSpec(memory_space=pltpu.VMEM),
            scratch_shapes=[
                pltpu.VMEM((2, tokens, feats), jnp.bfloat16),
                pltpu.VMEM((n_pieces, d_model, PC), jnp.bfloat16),
                pltpu.VMEM((n_pieces, PC, feats), jnp.bfloat16),
                pltpu.VMEM((tokens, d_model), jnp.bfloat16),
                pltpu.VMEM((tokens, feats), jnp.float32),
                pltpu.VMEM((2, 1, feats), jnp.float32),
                pltpu.SemaphoreType.DMA((10,)),
                pltpu.SemaphoreType.DMA((4,)),
                pltpu.SemaphoreType.DMA((N_RECV,)),
            ],
            compiler_params=pltpu.CompilerParams(collective_id=0, has_side_effects=True, vmem_limit_bytes=52000000),
        )(*[pltpu.with_memory_space_constraint(a, pltpu.HBM) for a in ins])
        return y.reshape(x_blk.shape)

    return jax.shard_map(per_device, mesh=mesh, in_specs=(act_spec, P("col"), P("row", "col"), P("row", "col")), out_specs=act_spec, check_vma=False)
```

```python
import jax
import jax.numpy as jnp
from jax import lax
from jax.experimental import pallas as pl
from jax.experimental.pallas import tpu as pltpu
from jax.sharding import PartitionSpec as P

LN_EPS = 1e-5
MESH = pl.DeviceIdType.MESH
PC = 256
SQRT_2_OVER_PI = 0.7978845608028654
X_ROWS = ((0, 512), (512, 512), (1024, 512), (1536, 384), (1920, 128))

A_ICI, A_D2D, B_Y, B_X, B_D2D, X_Y, G_Y = 0, 4, 8, 24, 32, 40, 45
N_RECV = 46
S_W1, S_W2, S_X, S_G = 0, 1, 2, 3


def gelu(u):
    inner = u * (SQRT_2_OVER_PI + (SQRT_2_OVER_PI * 0.044715) * (u * u))
    return ((0.5 * u) * (1.0 + jnp.tanh(inner))).astype(jnp.bfloat16)


def kernel(x_hbm, g_hbm, w1_hbm, w2_hbm, ys, xs, w1s, w2s, zs, acc, gs, load_sem, send_sem, recv_sem):
    rows1 = w1_hbm.shape[0]
    tokens, d_model = zs.shape
    half_d = d_model // 2

    col = lax.axis_index("col")
    row = lax.axis_index("row")
    core = row % 2
    row_p = row + 1 - 2 * core
    row_x = (row + 2) % 4
    row_xp = (row_p + 2) % 4
    other = 1 - col
    partner, x_nbr, y_nbr = {"row": row_p}, {"row": row_x}, {"col": other}

    def w1p(half, e, r, n=1):
        return w1s.at[pl.ds(half * 8 + e, n), pl.ds(pl.multiple_of(r * rows1, rows1), rows1)]

    def w2p(r, j):
        return w2s.at[(r // 2) * 8 + 2 * j + r % 2]

    def send(ref, dev, s_sem, r_sem):
        pltpu.make_async_remote_copy(
            src_ref=ref, dst_ref=ref, send_sem=send_sem.at[s_sem], recv_sem=recv_sem.at[r_sem],
            device_id=dev, device_id_type=MESH).start()

    def wait(ref, sem):
        pltpu.make_async_copy(ref, ref, sem).wait()

    def load_w(s):
        for e in (2 * s, 2 * s + 1):
            cols = pl.ds((e % 2) * (4 * PC) + (e // 2) * PC, PC)
            dst = w1s.at[col * 8 + e, pl.ds(pl.multiple_of(row * rows1, rows1), rows1)]
            pltpu.make_async_copy(w1_hbm.at[:, cols], dst, load_sem.at[s]).start()
        pltpu.make_async_copy(w2_hbm.at[pl.ds(s * PC, PC)], w2p(row, s), load_sem.at[s]).start()

    def x_part(h, i):
        r0, n = X_ROWS[i]
        return xs.at[h, pl.ds(r0, n)]

    def load_x(i):
        r0, n = X_ROWS[i]
        pltpu.make_async_copy(x_hbm.at[pl.ds(r0, n)], x_part(col, i), load_sem.at[4 + i]).start()

    pltpu.make_async_copy(g_hbm, gs.at[col], load_sem.at[9]).start()
    for s in range(4):
        load_w(s)
        load_x(s)
    load_x(4)

    barrier = pltpu.get_barrier_semaphore()
    for dev in (partner, x_nbr, y_nbr):
        pl.semaphore_signal(barrier, inc=1, device_id=dev, device_id_type=MESH)
    pl.semaphore_wait(barrier, 3)

    def send_x(i):
        wait(x_part(col, i), load_sem.at[4 + i])
        send(x_part(col, i), y_nbr, S_X, X_Y + i)

    def issue(s):
        wait(w1s.at[0], load_sem.at[s])
        w1, w2 = w1p(col, 2 * s, row, 2), w2p(row, s)
        send(w1, x_nbr, S_W1, A_ICI + s)
        send(w2, x_nbr, S_W2, A_ICI + s)
        send(w1, partner, S_W1, A_D2D + s)
        send(w2, partner, S_W2, A_D2D + s)
        send_x(s)

    def relay_a(s):
        wait(w1s.at[0], recv_sem.at[A_ICI + s])
        send(w1p(col, 2 * s, row_x, 2), partner, S_W1, A_D2D + s)
        send(w2p(row_x, s), partner, S_W2, A_D2D + s)

    def half_piece(half, e, h):
        return w1s.at[half * 8 + e, pl.ds(pl.multiple_of(row * rows1 + h * (rows1 // 2), rows1 // 2), rows1 // 2)]

    def relay_by(e, h):
        part = half_piece(other, e, h)
        wait(part, recv_sem.at[B_Y + 2 * e + h])
        send(part, x_nbr, S_W1, B_X + e)
        send(part, partner, S_W1, B_D2D + e)

    def relay_bx(e):
        wait(w1p(other, e, row_x), recv_sem.at[B_X + e])
        send(w1p(other, e, row_x), partner, S_W1, B_D2D + e)

    def layer_norm(i):
        r0, n = X_ROWS[i]
        rb = 64
        wait(x_part(other, i), recv_sem.at[X_Y + i])

        def step(t, _):
            rows = pl.ds(pl.multiple_of(r0 + t * rb, rb), rb)
            parts = [xs[h, rows, :].astype(jnp.float32) for h in range(2)]
            mean = sum(jnp.sum(v, axis=-1, keepdims=True) for v in parts) / d_model
            var = sum(jnp.sum(v * v, axis=-1, keepdims=True) for v in parts) / d_model - mean * mean
            inv = lax.rsqrt(var + LN_EPS)
            for h in range(2):
                zs[rows, h * half_d:(h + 1) * half_d] = ((parts[h] - mean) * inv * gs[h]).astype(jnp.bfloat16)
            acc[rows, :] = xs[col, rows, :].astype(jnp.float32)
            return 0

        lax.fori_loop(0, n // rb, step, 0)

    def sweep(units, store=None):
        held = None

        def finish():
            r0, n, ps, hs = held
            rows = pl.ds(r0, n)
            out = None
            for p, h in zip(ps, hs):
                term = jnp.dot(h, w2s[p], preferred_element_type=jnp.float32)
                out = term if out is None else out + term
            if store is None:
                acc[rows, :] += out
            else:
                store(rows, acc[rows, :] + out)

        for r0, n, ps in units:
            z = zs[pl.ds(r0, n), :]
            hs = [gelu(jnp.dot(z, w1s[p], preferred_element_type=jnp.float32)) for p in ps]
            if held is not None:
                finish()
            held = (r0, n, ps, hs)
        finish()

    def pieces(half, lo, hi):
        return [half * 8 + e for e in range(lo, hi)]

    with jax.named_scope("issue"):
        wait(gs.at[col], load_sem.at[9])
        send(gs.at[col], y_nbr, S_G, G_Y)
        issue(0)
        issue(1)
        wait(gs.at[other], recv_sem.at[G_Y])
    for s in range(3):
        with jax.named_scope(f"a_wait_x{s}"):
            if s < 2:
                issue(s + 2)
            if s == 1:
                for e in range(8):
                    for h in range(2):
                        send(half_piece(col, e, h), y_nbr, S_W1, B_Y + 2 * e + h)
                send_x(4)
            relay_a(s)
        with jax.named_scope(f"a_norm{s}"):
            layer_norm(s)
        with jax.named_scope(f"a_wait_d{s}"):
            wait(w1s.at[pl.ds(0, 2)], recv_sem.at[A_D2D + s])
        with jax.named_scope(f"a_tiles{s}"):
            def a_tile(t, _):
                q = t // (s + 1)
                g, j = t - q * (t - s), s - q * (t - s)
                p = col * 8 + 2 * j
                sweep([(pl.multiple_of(g * 512 + k, 256), 256, (p, p + 1)) for k in (0, 256)])
                return 0

            lax.fori_loop(0, 2 * s + 1, a_tile, 0)

    early = X_ROWS[4][0]
    third = early // 3
    with jax.named_scope("a_norm3"):
        layer_norm(3)
    def b_sweep(e, lo, hi, n=early // 4):
        return [(r, n, (other * 8 + e,)) for r in range(lo, hi, n)]

    def b_arrived(e):
        wait(w2s.at[0], recv_sem.at[B_D2D + e])

    with jax.named_scope("s0_a"):
        sweep([(*X_ROWS[3], pieces(col, 0, 2))])
    with jax.named_scope("s1"):
        relay_by(0, 0)
    with jax.named_scope("s1_a"):
        sweep([(*X_ROWS[3], pieces(col, e, e + 2)) for e in (2, 4)])
    with jax.named_scope("s2"):
        relay_by(0, 1)
        relay_a(3)
    with jax.named_scope("s2_d"):
        wait(w1s.at[pl.ds(0, 2)], recv_sem.at[A_D2D + 3])
    for q in range(3):
        with jax.named_scope(f"s{q + 3}_a"):
            sweep([(q * third + r, third // 2, pieces(col, 6, 8)) for r in (0, third // 2)])
        with jax.named_scope(f"s{q + 3}"):
            if q < 2:
                relay_by(1, q)
            if q == 1:
                relay_bx(0)
                relay_by(2, 0)

    def b_step(e, _):
        with jax.named_scope("s_odd"):
            relay_by(e + 2, 1)
        with jax.named_scope("s_odd_d"):
            b_arrived(e)
        with jax.named_scope("s_odd_b"):
            sweep(b_sweep(e, 0, early // 2))
        with jax.named_scope("s_even_x"):
            relay_bx(e + 1)
        with jax.named_scope("s_even"):
            relay_by(e + 3, 0)
        with jax.named_scope("s_even_b"):
            sweep(b_sweep(e, early // 2, early))
        return 0

    lax.fori_loop(0, 5, b_step, 0)
    with jax.named_scope("t_wait5"):
        relay_by(7, 1)
        relay_bx(6)
        b_arrived(5)
    with jax.named_scope("t_b5"):
        sweep(b_sweep(5, 0, early))
    with jax.named_scope("t_wait6"):
        b_arrived(6)
    with jax.named_scope("t_b6"):
        sweep(b_sweep(6, 0, early))
    with jax.named_scope("t_wait7"):
        relay_bx(7)
    with jax.named_scope("c_norm"):
        layer_norm(4)
    with jax.named_scope("c_tiles"):
        last = (pieces(col, 0, 8) + pieces(other, 0, 7))
        sweep([(early, tokens - early, last[k:k + 2]) for k in range(0, len(last), 2)])
    with jax.named_scope("d_wait"):
        wait(w2s.at[0], recv_sem.at[B_D2D + 7])
    with jax.named_scope("d_tile"):
        def write(rows, value):
            ys[rows, :] = value.astype(jnp.bfloat16)

        sweep([(r, tokens // 4, (other * 8 + 7,)) for r in range(0, tokens, tokens // 4)], write)

    with jax.named_scope("sent"):
        wait(w1s.at[pl.ds(0, 14)], send_sem.at[S_W1])
        wait(w2s.at[pl.ds(0, 12)], send_sem.at[S_W2])
        wait(xs.at[0], send_sem.at[S_X])
        wait(gs.at[0], send_sem.at[S_G])


def solution(mesh):
    act_spec = P(None, ("dp", "row"), "col")

    def per_device(x_blk, gamma_blk, w_in_blk, w_out_blk):
        feats = x_blk.shape[2]
        tokens = x_blk.shape[0] * x_blk.shape[1]
        d_model = 2 * feats
        n_pieces = 2 * w_in_blk.shape[1] // PC
        ins = (x_blk.reshape(tokens, feats), gamma_blk.reshape(1, feats), w_in_blk, w_out_blk)
        y = pl.pallas_call(
            kernel,
            name="mlp",
            out_shape=jax.ShapeDtypeStruct((tokens, feats), jnp.bfloat16),
            in_specs=[pl.BlockSpec(memory_space=pltpu.HBM)] * 4,
            out_specs=pl.BlockSpec(memory_space=pltpu.VMEM),
            scratch_shapes=[
                pltpu.VMEM((2, tokens, feats), jnp.bfloat16),
                pltpu.VMEM((n_pieces, d_model, PC), jnp.bfloat16),
                pltpu.VMEM((n_pieces, PC, feats), jnp.bfloat16),
                pltpu.VMEM((tokens, d_model), jnp.bfloat16),
                pltpu.VMEM((tokens, feats), jnp.float32),
                pltpu.VMEM((2, 1, feats), jnp.float32),
                pltpu.SemaphoreType.DMA((10,)),
                pltpu.SemaphoreType.DMA((4,)),
                pltpu.SemaphoreType.DMA((N_RECV,)),
            ],
            compiler_params=pltpu.CompilerParams(collective_id=0, has_side_effects=True, vmem_limit_bytes=52000000),
        )(*[pltpu.with_memory_space_constraint(a, pltpu.HBM) for a in ins])
        return y.reshape(x_blk.shape)

    return jax.shard_map(per_device, mesh=mesh, in_specs=(act_spec, P("col"), P("row", "col"), P("row", "col")), out_specs=act_spec, check_vma=False)
```

```python
import jax
import jax.numpy as jnp
from jax import lax
from jax.experimental import pallas as pl
from jax.experimental.pallas import tpu as pltpu
from jax.sharding import PartitionSpec as P

LN_EPS = 1e-5
MESH = pl.DeviceIdType.MESH
PC = 256
SQRT_2_OVER_PI = 0.7978845608028654
X_ROWS = ((0, 512), (512, 512), (1024, 512), (1536, 384), (1920, 128))

A_ICI, A_D2D, B_Y, B_X, B_D2D, X_Y, G_Y = 0, 4, 8, 24, 32, 40, 45
N_RECV = 46
S_W1, S_W2, S_X, S_G = 0, 1, 2, 3


def gelu(u):
    inner = u * (SQRT_2_OVER_PI + (SQRT_2_OVER_PI * 0.044715) * (u * u))
    return ((0.5 * u) * (1.0 + jnp.tanh(inner))).astype(jnp.bfloat16)


def kernel(x_hbm, g_hbm, w1_hbm, w2_hbm, ys, xs, w1s, w2s, zs, acc, gs, load_sem, send_sem, recv_sem):
    rows1 = w1_hbm.shape[0]
    tokens, d_model = zs.shape
    half_d = d_model // 2

    col = lax.axis_index("col")
    row = lax.axis_index("row")
    core = row % 2
    row_p = row + 1 - 2 * core
    row_x = (row + 2) % 4
    row_xp = (row_p + 2) % 4
    other = 1 - col
    partner, x_nbr, y_nbr = {"row": row_p}, {"row": row_x}, {"col": other}

    def w1p(half, e, r, n=1):
        return w1s.at[pl.ds(half * 8 + e, n), pl.ds(pl.multiple_of(r * rows1, rows1), rows1)]

    def w2p(r, j):
        return w2s.at[(r // 2) * 8 + 2 * j + r % 2]

    def send(ref, dev, s_sem, r_sem):
        pltpu.make_async_remote_copy(
            src_ref=ref, dst_ref=ref, send_sem=send_sem.at[s_sem], recv_sem=recv_sem.at[r_sem],
            device_id=dev, device_id_type=MESH).start()

    def wait(ref, sem):
        pltpu.make_async_copy(ref, ref, sem).wait()

    def load_w(s):
        for e in (2 * s, 2 * s + 1):
            cols = pl.ds((e % 2) * (4 * PC) + (e // 2) * PC, PC)
            dst = w1s.at[col * 8 + e, pl.ds(pl.multiple_of(row * rows1, rows1), rows1)]
            pltpu.make_async_copy(w1_hbm.at[:, cols], dst, load_sem.at[s]).start()
        pltpu.make_async_copy(w2_hbm.at[pl.ds(s * PC, PC)], w2p(row, s), load_sem.at[s]).start()

    def x_part(h, i):
        r0, n = X_ROWS[i]
        return xs.at[h, pl.ds(r0, n)]

    def load_x(i):
        r0, n = X_ROWS[i]
        pltpu.make_async_copy(x_hbm.at[pl.ds(r0, n)], x_part(col, i), load_sem.at[4 + i]).start()

    pltpu.make_async_copy(g_hbm, gs.at[col], load_sem.at[9]).start()
    for s in range(4):
        load_w(s)
        load_x(s)
    load_x(4)

    barrier = pltpu.get_barrier_semaphore()
    for dev in (partner, x_nbr, y_nbr):
        pl.semaphore_signal(barrier, inc=1, device_id=dev, device_id_type=MESH)
    pl.semaphore_wait(barrier, 3)

    def send_x(i):
        wait(x_part(col, i), load_sem.at[4 + i])
        send(x_part(col, i), y_nbr, S_X, X_Y + i)

    def issue(s):
        wait(w1s.at[0], load_sem.at[s])
        w1, w2 = w1p(col, 2 * s, row, 2), w2p(row, s)
        send(w1, x_nbr, S_W1, A_ICI + s)
        send(w2, x_nbr, S_W2, A_ICI + s)
        send(w1, partner, S_W1, A_D2D + s)
        send(w2, partner, S_W2, A_D2D + s)
        send_x(s)

    def relay_a(s):
        wait(w1s.at[0], recv_sem.at[A_ICI + s])
        send(w1p(col, 2 * s, row_x, 2), partner, S_W1, A_D2D + s)
        send(w2p(row_x, s), partner, S_W2, A_D2D + s)

    def half_piece(half, e, h):
        return w1s.at[half * 8 + e, pl.ds(pl.multiple_of(row * rows1 + h * (rows1 // 2), rows1 // 2), rows1 // 2)]

    def relay_by(e, h):
        part = half_piece(other, e, h)
        wait(part, recv_sem.at[B_Y + 2 * e + h])
        send(part, x_nbr, S_W1, B_X + e)
        send(part, partner, S_W1, B_D2D + e)

    def relay_bx(e):
        wait(w1p(other, e, row_x), recv_sem.at[B_X + e])
        send(w1p(other, e, row_x), partner, S_W1, B_D2D + e)

    def layer_norm(i):
        r0, n = X_ROWS[i]
        rb = 64
        wait(x_part(other, i), recv_sem.at[X_Y + i])

        def step(t, _):
            rows = pl.ds(pl.multiple_of(r0 + t * rb, rb), rb)
            parts = [xs[h, rows, :].astype(jnp.float32) for h in range(2)]
            mean = sum(jnp.sum(v, axis=-1, keepdims=True) for v in parts) / d_model
            var = sum(jnp.sum(v * v, axis=-1, keepdims=True) for v in parts) / d_model - mean * mean
            inv = lax.rsqrt(var + LN_EPS)
            for h in range(2):
                zs[rows, h * half_d:(h + 1) * half_d] = ((parts[h] - mean) * inv * gs[h]).astype(jnp.bfloat16)
            acc[rows, :] = xs[col, rows, :].astype(jnp.float32)
            return 0

        lax.fori_loop(0, n // rb, step, 0)

    held = []

    def finish():
        if held:
            r0, n, ps, hs, store = held.pop()
            rows = pl.ds(r0, n)
            out = None
            for p, h in zip(ps, hs):
                term = jnp.dot(h, w2s[p], preferred_element_type=jnp.float32)
                out = term if out is None else out + term
            if store is None:
                acc[rows, :] += out
            else:
                store(rows, acc[rows, :] + out)

    def unit(r0, n, ps, store=None):
        z = zs[pl.ds(r0, n), :]
        hs = [gelu(jnp.dot(z, w1s[p], preferred_element_type=jnp.float32)) for p in ps]
        finish()
        held.append((r0, n, ps, hs, store))

    def pieces(half, lo, hi):
        return [half * 8 + e for e in range(lo, hi)]

    with jax.named_scope("issue"):
        wait(gs.at[col], load_sem.at[9])
        send(gs.at[col], y_nbr, S_G, G_Y)
        issue(0)
        issue(1)
        wait(gs.at[other], recv_sem.at[G_Y])
    for s in range(3):
        with jax.named_scope(f"a_wait_x{s}"):
            if s < 2:
                issue(s + 2)
            if s == 1:
                for e in range(8):
                    for h in range(2):
                        send(half_piece(col, e, h), y_nbr, S_W1, B_Y + 2 * e + h)
                send_x(4)
            relay_a(s)
        with jax.named_scope(f"a_norm{s}"):
            layer_norm(s)
        with jax.named_scope(f"a_wait_d{s}"):
            wait(w1s.at[pl.ds(0, 2)], recv_sem.at[A_D2D + s])
        with jax.named_scope(f"a_tiles{s}"):
            def a_tile(t, _):
                q = t // (s + 1)
                g, j = t - q * (t - s), s - q * (t - s)
                p = col * 8 + 2 * j
                for k in (0, 256):
                    unit(pl.multiple_of(g * 512 + k, 256), 256, (p, p + 1))
                finish()
                return 0

            lax.fori_loop(0, 2 * s + 1, a_tile, 0)

    early = X_ROWS[4][0]
    third = early // 3
    with jax.named_scope("a_norm3"):
        layer_norm(3)
    quarter = early // 4

    def first(e):
        with jax.named_scope(f"first{e}"):
            unit(*X_ROWS[3], pieces(col, 2 * e, 2 * e + 2))

    def a_unit(q):
        unit(q * quarter, quarter, pieces(col, 6, 8))

    def b_unit(e, q):
        unit(q * quarter, quarter, pieces(other, e, e + 1))

    def by(e, h):
        with jax.named_scope(f"by{e}{h}"):
            relay_by(e, h)

    def bx(e):
        with jax.named_scope(f"bx{e}"):
            relay_bx(e)

    def b_arrived(e):
        with jax.named_scope(f"bd{e}"):
            wait(w2s.at[0], recv_sem.at[B_D2D + e])

    first(0)
    by(0, 0)
    first(1)
    first(2)
    by(0, 1)
    with jax.named_scope("a3"):
        relay_a(3)
    by(1, 0)
    with jax.named_scope("ad3"):
        wait(w1s.at[pl.ds(0, 2)], recv_sem.at[A_D2D + 3])
    a_unit(0)
    by(1, 1)
    a_unit(1)
    bx(0)
    a_unit(2)
    by(2, 0)
    a_unit(3)
    by(2, 1)
    bx(1)
    b_arrived(0)
    for q in range(3):
        b_unit(0, q)
    by(3, 0)
    b_unit(0, 3)
    b_arrived(1)
    b_unit(1, 0)
    b_unit(1, 1)
    by(3, 1)
    bx(2)
    b_unit(1, 2)
    b_unit(1, 3)
    for e in range(2, 6):
        by(e + 2, 0)
        b_arrived(e)
        b_unit(e, 0)
        b_unit(e, 1)
        by(e + 2, 1)
        bx(e + 1)
        b_unit(e, 2)
        b_unit(e, 3)
    b_arrived(6)
    for q in range(3):
        b_unit(6, q)
    bx(7)
    b_unit(6, 3)
    with jax.named_scope("c_norm"):
        layer_norm(4)
    with jax.named_scope("c_tiles"):
        last = pieces(col, 0, 8) + pieces(other, 0, 7)
        for k in range(0, len(last), 2):
            unit(early, tokens - early, last[k:k + 2])
        finish()
    b_arrived(7)
    with jax.named_scope("d_tile"):
        def write(rows, value):
            ys[rows, :] = value.astype(jnp.bfloat16)

        for q in range(4):
            unit(q * (tokens // 4), tokens // 4, pieces(other, 7, 8), write)
        finish()

    with jax.named_scope("sent"):
        wait(w1s.at[pl.ds(0, 14)], send_sem.at[S_W1])
        wait(w2s.at[pl.ds(0, 12)], send_sem.at[S_W2])
        wait(xs.at[0], send_sem.at[S_X])
        wait(gs.at[0], send_sem.at[S_G])


def solution(mesh):
    act_spec = P(None, ("dp", "row"), "col")

    def per_device(x_blk, gamma_blk, w_in_blk, w_out_blk):
        feats = x_blk.shape[2]
        tokens = x_blk.shape[0] * x_blk.shape[1]
        d_model = 2 * feats
        n_pieces = 2 * w_in_blk.shape[1] // PC
        ins = (x_blk.reshape(tokens, feats), gamma_blk.reshape(1, feats), w_in_blk, w_out_blk)
        y = pl.pallas_call(
            kernel,
            name="mlp",
            out_shape=jax.ShapeDtypeStruct((tokens, feats), jnp.bfloat16),
            in_specs=[pl.BlockSpec(memory_space=pltpu.HBM)] * 4,
            out_specs=pl.BlockSpec(memory_space=pltpu.VMEM),
            scratch_shapes=[
                pltpu.VMEM((2, tokens, feats), jnp.bfloat16),
                pltpu.VMEM((n_pieces, d_model, PC), jnp.bfloat16),
                pltpu.VMEM((n_pieces, PC, feats), jnp.bfloat16),
                pltpu.VMEM((tokens, d_model), jnp.bfloat16),
                pltpu.VMEM((tokens, feats), jnp.float32),
                pltpu.VMEM((2, 1, feats), jnp.float32),
                pltpu.SemaphoreType.DMA((10,)),
                pltpu.SemaphoreType.DMA((4,)),
                pltpu.SemaphoreType.DMA((N_RECV,)),
            ],
            compiler_params=pltpu.CompilerParams(collective_id=0, has_side_effects=True, vmem_limit_bytes=52000000),
        )(*[pltpu.with_memory_space_constraint(a, pltpu.HBM) for a in ins])
        return y.reshape(x_blk.shape)

    return jax.shard_map(per_device, mesh=mesh, in_specs=(act_spec, P("col"), P("row", "col"), P("row", "col")), out_specs=act_spec, check_vma=False)
```

```python
import jax
import jax.numpy as jnp
from jax import lax
from jax.experimental import pallas as pl
from jax.experimental.pallas import tpu as pltpu
from jax.sharding import PartitionSpec as P

LN_EPS = 1e-5
MESH = pl.DeviceIdType.MESH
PC = 256
SQRT_2_OVER_PI = 0.7978845608028654
X_ROWS = ((0, 512), (512, 512), (1024, 512), (1536, 320), (1856, 192))

A_ICI, A_D2D, B_Y, B_X, B_D2D, X_Y, G_Y = 0, 4, 8, 24, 32, 40, 45
N_RECV = 46
S_W1, S_W2, S_X, S_G = 0, 1, 2, 3


def gelu(u):
    inner = u * (SQRT_2_OVER_PI + (SQRT_2_OVER_PI * 0.044715) * (u * u))
    return ((0.5 * u) * (1.0 + jnp.tanh(inner))).astype(jnp.bfloat16)


def kernel(x_hbm, g_hbm, w1_hbm, w2_hbm, ys, xs, w1s, w2s, zs, acc, gs, load_sem, send_sem, recv_sem):
    rows1 = w1_hbm.shape[0]
    tokens, d_model = zs.shape
    half_d = d_model // 2

    col = lax.axis_index("col")
    row = lax.axis_index("row")
    core = row % 2
    row_p = row + 1 - 2 * core
    row_x = (row + 2) % 4
    row_xp = (row_p + 2) % 4
    other = 1 - col
    partner, x_nbr, y_nbr = {"row": row_p}, {"row": row_x}, {"col": other}

    def w1p(half, e, r, n=1):
        return w1s.at[pl.ds(half * 8 + e, n), pl.ds(pl.multiple_of(r * rows1, rows1), rows1)]

    def w2p(r, j):
        return w2s.at[(r // 2) * 8 + 2 * j + r % 2]

    def send(ref, dev, s_sem, r_sem):
        pltpu.make_async_remote_copy(
            src_ref=ref, dst_ref=ref, send_sem=send_sem.at[s_sem], recv_sem=recv_sem.at[r_sem],
            device_id=dev, device_id_type=MESH).start()

    def wait(ref, sem):
        pltpu.make_async_copy(ref, ref, sem).wait()

    def load_w(s):
        for e in (2 * s, 2 * s + 1):
            cols = pl.ds((e % 2) * (4 * PC) + (e // 2) * PC, PC)
            dst = w1s.at[col * 8 + e, pl.ds(pl.multiple_of(row * rows1, rows1), rows1)]
            pltpu.make_async_copy(w1_hbm.at[:, cols], dst, load_sem.at[s]).start()
        pltpu.make_async_copy(w2_hbm.at[pl.ds(s * PC, PC)], w2p(row, s), load_sem.at[s]).start()

    def x_part(h, i):
        r0, n = X_ROWS[i]
        return xs.at[h, pl.ds(r0, n)]

    def load_x(i):
        r0, n = X_ROWS[i]
        pltpu.make_async_copy(x_hbm.at[pl.ds(r0, n)], x_part(col, i), load_sem.at[4 + i]).start()

    pltpu.make_async_copy(g_hbm, gs.at[col], load_sem.at[9]).start()
    for s in range(4):
        load_w(s)
        load_x(s)
    load_x(4)

    barrier = pltpu.get_barrier_semaphore()
    for dev in (partner, x_nbr, y_nbr):
        pl.semaphore_signal(barrier, inc=1, device_id=dev, device_id_type=MESH)
    pl.semaphore_wait(barrier, 3)

    def send_x(i):
        wait(x_part(col, i), load_sem.at[4 + i])
        send(x_part(col, i), y_nbr, S_X, X_Y + i)

    def issue(s):
        wait(w1s.at[0], load_sem.at[s])
        w1, w2 = w1p(col, 2 * s, row, 2), w2p(row, s)
        send(w1, x_nbr, S_W1, A_ICI + s)
        send(w2, x_nbr, S_W2, A_ICI + s)
        send(w1, partner, S_W1, A_D2D + s)
        send(w2, partner, S_W2, A_D2D + s)
        send_x(s)

    def relay_a(s):
        wait(w1s.at[0], recv_sem.at[A_ICI + s])
        send(w1p(col, 2 * s, row_x, 2), partner, S_W1, A_D2D + s)
        send(w2p(row_x, s), partner, S_W2, A_D2D + s)

    def half_piece(half, e, h):
        return w1s.at[half * 8 + e, pl.ds(pl.multiple_of(row * rows1 + h * (rows1 // 2), rows1 // 2), rows1 // 2)]

    def relay_by(e, h):
        part = half_piece(other, e, h)
        wait(part, recv_sem.at[B_Y + 2 * e + h])
        send(part, x_nbr, S_W1, B_X + e)
        send(part, partner, S_W1, B_D2D + e)

    def relay_bx(e):
        wait(w1p(other, e, row_x), recv_sem.at[B_X + e])
        send(w1p(other, e, row_x), partner, S_W1, B_D2D + e)

    def layer_norm(i):
        r0, n = X_ROWS[i]
        rb = 64
        wait(x_part(other, i), recv_sem.at[X_Y + i])

        def step(t, _):
            rows = pl.ds(pl.multiple_of(r0 + t * rb, rb), rb)
            parts = [xs[h, rows, :].astype(jnp.float32) for h in range(2)]
            mean = sum(jnp.sum(v, axis=-1, keepdims=True) for v in parts) / d_model
            var = sum(jnp.sum(v * v, axis=-1, keepdims=True) for v in parts) / d_model - mean * mean
            inv = lax.rsqrt(var + LN_EPS)
            for h in range(2):
                zs[rows, h * half_d:(h + 1) * half_d] = ((parts[h] - mean) * inv * gs[h]).astype(jnp.bfloat16)
            acc[rows, :] = xs[col, rows, :].astype(jnp.float32)
            return 0

        lax.fori_loop(0, n // rb, step, 0)

    held = []

    def finish():
        if held:
            r0, n, ps, hs, store = held.pop()
            rows = pl.ds(r0, n)
            out = None
            for p, h in zip(ps, hs):
                term = jnp.dot(h, w2s[p], preferred_element_type=jnp.float32)
                out = term if out is None else out + term
            if store is None:
                acc[rows, :] += out
            else:
                store(rows, acc[rows, :] + out)

    def unit(r0, n, ps, store=None):
        z = zs[pl.ds(r0, n), :]
        hs = [gelu(jnp.dot(z, w1s[p], preferred_element_type=jnp.float32)) for p in ps]
        finish()
        held.append((r0, n, ps, hs, store))

    def pieces(half, lo, hi):
        return [half * 8 + e for e in range(lo, hi)]

    with jax.named_scope("issue"):
        wait(gs.at[col], load_sem.at[9])
        send(gs.at[col], y_nbr, S_G, G_Y)
        issue(0)
        issue(1)
        wait(gs.at[other], recv_sem.at[G_Y])
    for s in range(3):
        with jax.named_scope(f"a_wait_x{s}"):
            if s < 2:
                issue(s + 2)
            if s == 1:
                for e in range(8):
                    for h in range(2):
                        send(half_piece(col, e, h), y_nbr, S_W1, B_Y + 2 * e + h)
                send_x(4)
            relay_a(s)
        with jax.named_scope(f"a_norm{s}"):
            layer_norm(s)
        with jax.named_scope(f"a_wait_d{s}"):
            wait(w1s.at[pl.ds(0, 2)], recv_sem.at[A_D2D + s])
        with jax.named_scope(f"a_tiles{s}"):
            def a_tile(t, _):
                q = t // (s + 1)
                g, j = t - q * (t - s), s - q * (t - s)
                p = col * 8 + 2 * j
                for k in (0, 256):
                    unit(pl.multiple_of(g * 512 + k, 256), 256, (p, p + 1))
                finish()
                return 0

            lax.fori_loop(0, 2 * s + 1, a_tile, 0)

    early = X_ROWS[4][0]
    third = early // 3
    with jax.named_scope("a_norm3"):
        layer_norm(3)
    quarter = early // 4

    def first(e):
        with jax.named_scope(f"first{e}"):
            unit(*X_ROWS[3], pieces(col, 2 * e, 2 * e + 2))

    def a_unit(q):
        unit(q * quarter, quarter, pieces(col, 6, 8))

    def b_unit(e, q):
        unit(q * quarter, quarter, pieces(other, e, e + 1))

    def by(e, h):
        with jax.named_scope(f"by{e}{h}"):
            relay_by(e, h)

    def bx(e):
        with jax.named_scope(f"bx{e}"):
            relay_bx(e)

    def b_arrived(e):
        with jax.named_scope(f"bd{e}"):
            wait(w2s.at[0], recv_sem.at[B_D2D + e])

    first(0)
    by(0, 0)
    first(1)
    first(2)
    by(0, 1)
    with jax.named_scope("a3"):
        relay_a(3)
    by(1, 0)
    with jax.named_scope("ad3"):
        wait(w1s.at[pl.ds(0, 2)], recv_sem.at[A_D2D + 3])
    a_unit(0)
    by(1, 1)
    a_unit(1)
    a_unit(2)
    bx(0)
    by(2, 0)
    a_unit(3)
    for e in range(5):
        by(e + 2, 1)
        b_arrived(e)
        b_unit(e, 0)
        b_unit(e, 1)
        bx(e + 1)
        by(e + 3, 0)
        b_unit(e, 2)
        b_unit(e, 3)
    by(7, 1)
    b_arrived(5)
    b_unit(5, 0)
    b_unit(5, 1)
    bx(6)
    b_unit(5, 2)
    b_unit(5, 3)
    b_arrived(6)
    for q in range(3):
        b_unit(6, q)
    bx(7)
    b_unit(6, 3)
    with jax.named_scope("c_norm"):
        layer_norm(4)
    with jax.named_scope("c_tiles"):
        last = pieces(col, 0, 8) + pieces(other, 0, 7)
        for k in range(0, len(last), 2):
            unit(early, tokens - early, last[k:k + 2])
        finish()
    b_arrived(7)
    with jax.named_scope("d_tile"):
        def write(rows, value):
            ys[rows, :] = value.astype(jnp.bfloat16)

        for q in range(4):
            unit(q * (tokens // 4), tokens // 4, pieces(other, 7, 8), write)
        finish()

    with jax.named_scope("sent"):
        wait(w1s.at[pl.ds(0, 14)], send_sem.at[S_W1])
        wait(w2s.at[pl.ds(0, 12)], send_sem.at[S_W2])
        wait(xs.at[0], send_sem.at[S_X])
        wait(gs.at[0], send_sem.at[S_G])


def solution(mesh):
    act_spec = P(None, ("dp", "row"), "col")

    def per_device(x_blk, gamma_blk, w_in_blk, w_out_blk):
        feats = x_blk.shape[2]
        tokens = x_blk.shape[0] * x_blk.shape[1]
        d_model = 2 * feats
        n_pieces = 2 * w_in_blk.shape[1] // PC
        ins = (x_blk.reshape(tokens, feats), gamma_blk.reshape(1, feats), w_in_blk, w_out_blk)
        y = pl.pallas_call(
            kernel,
            name="mlp",
            out_shape=jax.ShapeDtypeStruct((tokens, feats), jnp.bfloat16),
            in_specs=[pl.BlockSpec(memory_space=pltpu.HBM)] * 4,
            out_specs=pl.BlockSpec(memory_space=pltpu.VMEM),
            scratch_shapes=[
                pltpu.VMEM((2, tokens, feats), jnp.bfloat16),
                pltpu.VMEM((n_pieces, d_model, PC), jnp.bfloat16),
                pltpu.VMEM((n_pieces, PC, feats), jnp.bfloat16),
                pltpu.VMEM((tokens, d_model), jnp.bfloat16),
                pltpu.VMEM((tokens, feats), jnp.float32),
                pltpu.VMEM((2, 1, feats), jnp.float32),
                pltpu.SemaphoreType.DMA((10,)),
                pltpu.SemaphoreType.DMA((4,)),
                pltpu.SemaphoreType.DMA((N_RECV,)),
            ],
            compiler_params=pltpu.CompilerParams(collective_id=0, has_side_effects=True, vmem_limit_bytes=52000000),
        )(*[pltpu.with_memory_space_constraint(a, pltpu.HBM) for a in ins])
        return y.reshape(x_blk.shape)

    return jax.shard_map(per_device, mesh=mesh, in_specs=(act_spec, P("col"), P("row", "col"), P("row", "col")), out_specs=act_spec, check_vma=False)
```

```python
import jax
import jax.numpy as jnp
from jax import lax
from jax.experimental import pallas as pl
from jax.experimental.pallas import tpu as pltpu
from jax.sharding import PartitionSpec as P

LN_EPS = 1e-5
MESH = pl.DeviceIdType.MESH
PC = 256
SQRT_2_OVER_PI = 0.7978845608028654
X_ROWS = ((0, 512), (512, 512), (1024, 512), (1536, 320), (1856, 192))

A_ICI, A_D2D, B_Y, B_X, B_D2D, X_Y, G_Y = 0, 4, 8, 24, 32, 40, 45
N_RECV = 46
S_W1, S_W2, S_X, S_G = 0, 1, 2, 3


def gelu(u):
    inner = u * (SQRT_2_OVER_PI + (SQRT_2_OVER_PI * 0.044715) * (u * u))
    return ((0.5 * u) * (1.0 + jnp.tanh(inner))).astype(jnp.bfloat16)


def kernel(x_hbm, g_hbm, w1_hbm, w2_hbm, ys, xs, w1s, w2s, zs, acc, gs, load_sem, send_sem, recv_sem):
    rows1 = w1_hbm.shape[0]
    tokens, d_model = zs.shape
    half_d = d_model // 2

    col = lax.axis_index("col")
    row = lax.axis_index("row")
    core = row % 2
    row_p = row + 1 - 2 * core
    row_x = (row + 2) % 4
    row_xp = (row_p + 2) % 4
    other = 1 - col
    partner, x_nbr, y_nbr = {"row": row_p}, {"row": row_x}, {"col": other}

    def w1p(half, e, r, n=1):
        return w1s.at[pl.ds(half * 8 + e, n), pl.ds(pl.multiple_of(r * rows1, rows1), rows1)]

    def w2p(r, j):
        return w2s.at[(r // 2) * 8 + 2 * j + r % 2]

    def send(ref, dev, s_sem, r_sem):
        pltpu.make_async_remote_copy(
            src_ref=ref, dst_ref=ref, send_sem=send_sem.at[s_sem], recv_sem=recv_sem.at[r_sem],
            device_id=dev, device_id_type=MESH).start()

    def wait(ref, sem):
        pltpu.make_async_copy(ref, ref, sem).wait()

    def load_w(s):
        for e in (2 * s, 2 * s + 1):
            cols = pl.ds((e % 2) * (4 * PC) + (e // 2) * PC, PC)
            dst = w1s.at[col * 8 + e, pl.ds(pl.multiple_of(row * rows1, rows1), rows1)]
            pltpu.make_async_copy(w1_hbm.at[:, cols], dst, load_sem.at[s]).start()
        pltpu.make_async_copy(w2_hbm.at[pl.ds(s * PC, PC)], w2p(row, s), load_sem.at[s]).start()

    def x_part(h, i):
        r0, n = X_ROWS[i]
        return xs.at[h, pl.ds(r0, n)]

    def load_x(i):
        r0, n = X_ROWS[i]
        pltpu.make_async_copy(x_hbm.at[pl.ds(r0, n)], x_part(col, i), load_sem.at[4 + i]).start()

    pltpu.make_async_copy(g_hbm, gs.at[col], load_sem.at[9]).start()
    for s in range(4):
        load_w(s)
        load_x(s)
    load_x(4)

    barrier = pltpu.get_barrier_semaphore()
    for dev in (partner, x_nbr, y_nbr):
        pl.semaphore_signal(barrier, inc=1, device_id=dev, device_id_type=MESH)
    pl.semaphore_wait(barrier, 3)

    def send_x(i):
        wait(x_part(col, i), load_sem.at[4 + i])
        send(x_part(col, i), y_nbr, S_X, X_Y + i)

    def issue(s):
        wait(w1s.at[0], load_sem.at[s])
        w1, w2 = w1p(col, 2 * s, row, 2), w2p(row, s)
        send(w1, x_nbr, S_W1, A_ICI + s)
        send(w2, x_nbr, S_W2, A_ICI + s)
        send(w1, partner, S_W1, A_D2D + s)
        send(w2, partner, S_W2, A_D2D + s)
        send_x(s)

    def relay_a(s):
        wait(w1s.at[0], recv_sem.at[A_ICI + s])
        send(w1p(col, 2 * s, row_x, 2), partner, S_W1, A_D2D + s)
        send(w2p(row_x, s), partner, S_W2, A_D2D + s)

    def half_piece(half, e, h):
        return w1s.at[half * 8 + e, pl.ds(pl.multiple_of(row * rows1 + h * (rows1 // 2), rows1 // 2), rows1 // 2)]

    def relay_by(e, h):
        part = half_piece(other, e, h)
        wait(part, recv_sem.at[B_Y + 2 * e + h])
        send(part, x_nbr, S_W1, B_X + e)
        send(part, partner, S_W1, B_D2D + e)

    def relay_bx(e):
        wait(w1p(other, e, row_x), recv_sem.at[B_X + e])
        send(w1p(other, e, row_x), partner, S_W1, B_D2D + e)

    def layer_norm(i):
        r0, n = X_ROWS[i]
        rb = 64
        wait(x_part(other, i), recv_sem.at[X_Y + i])

        def step(t, _):
            rows = pl.ds(pl.multiple_of(r0 + t * rb, rb), rb)
            parts = [xs[h, rows, :].astype(jnp.float32) for h in range(2)]
            mean = sum(jnp.sum(v, axis=-1, keepdims=True) for v in parts) / d_model
            var = sum(jnp.sum(v * v, axis=-1, keepdims=True) for v in parts) / d_model - mean * mean
            inv = lax.rsqrt(var + LN_EPS)
            for h in range(2):
                zs[rows, h * half_d:(h + 1) * half_d] = ((parts[h] - mean) * inv * gs[h]).astype(jnp.bfloat16)
            acc[rows, :] = xs[col, rows, :].astype(jnp.float32)
            return 0

        lax.fori_loop(0, n // rb, step, 0, unroll=n <= 192)

    held = []

    def finish():
        if held:
            r0, n, ps, hs, store = held.pop()
            rows = pl.ds(r0, n)
            out = None
            for p, h in zip(ps, hs):
                term = jnp.dot(h, w2s[p], preferred_element_type=jnp.float32)
                out = term if out is None else out + term
            if store is None:
                acc[rows, :] += out
            else:
                store(rows, acc[rows, :] + out)

    def unit(r0, n, ps, store=None):
        z = zs[pl.ds(r0, n), :]
        hs = [gelu(jnp.dot(z, w1s[p], preferred_element_type=jnp.float32)) for p in ps]
        finish()
        held.append((r0, n, ps, hs, store))

    def pieces(half, lo, hi):
        return [half * 8 + e for e in range(lo, hi)]

    with jax.named_scope("issue"):
        wait(gs.at[col], load_sem.at[9])
        send(gs.at[col], y_nbr, S_G, G_Y)
        issue(0)
        issue(1)
        wait(gs.at[other], recv_sem.at[G_Y])
    for s in range(3):
        with jax.named_scope(f"a_wait_x{s}"):
            if s < 2:
                issue(s + 2)
            if s == 1:
                for e in range(8):
                    for h in range(2):
                        send(half_piece(col, e, h), y_nbr, S_W1, B_Y + 2 * e + h)
                send_x(4)
            relay_a(s)
        with jax.named_scope(f"a_norm{s}"):
            layer_norm(s)
        with jax.named_scope(f"a_wait_d{s}"):
            wait(w1s.at[pl.ds(0, 2)], recv_sem.at[A_D2D + s])
        with jax.named_scope(f"a_tiles{s}"):
            def a_tile(t, _):
                q = t // (s + 1)
                g, j = t - q * (t - s), s - q * (t - s)
                p = col * 8 + 2 * j
                for k in (0, 256):
                    unit(pl.multiple_of(g * 512 + k, 256), 256, (p, p + 1))
                finish()
                return 0

            lax.fori_loop(0, 2 * s + 1, a_tile, 0)

    early = X_ROWS[4][0]
    third = early // 3
    with jax.named_scope("a_norm3"):
        layer_norm(3)
    quarter = early // 4

    def first(e):
        with jax.named_scope(f"first{e}"):
            unit(*X_ROWS[3], pieces(col, 2 * e, 2 * e + 2))

    def a_unit(q):
        unit(q * quarter, quarter, pieces(col, 6, 8))

    def b_unit(e, q):
        unit(q * quarter, quarter, pieces(other, e, e + 1))

    def by(e, h):
        with jax.named_scope(f"by{e}{h}"):
            relay_by(e, h)

    def bx(e):
        with jax.named_scope(f"bx{e}"):
            relay_bx(e)

    def b_arrived(e):
        with jax.named_scope(f"bd{e}"):
            wait(w2s.at[0], recv_sem.at[B_D2D + e])

    first(0)
    by(0, 0)
    first(1)
    first(2)
    by(0, 1)
    with jax.named_scope("a3"):
        relay_a(3)
    by(1, 0)
    with jax.named_scope("ad3"):
        wait(w1s.at[pl.ds(0, 2)], recv_sem.at[A_D2D + 3])
    a_unit(0)
    by(1, 1)
    a_unit(1)
    a_unit(2)
    bx(0)
    by(2, 0)
    a_unit(3)
    for e in range(5):
        by(e + 2, 1)
        b_arrived(e)
        b_unit(e, 0)
        b_unit(e, 1)
        bx(e + 1)
        by(e + 3, 0)
        b_unit(e, 2)
        b_unit(e, 3)
    by(7, 1)
    b_arrived(5)
    b_unit(5, 0)
    b_unit(5, 1)
    bx(6)
    b_unit(5, 2)
    b_unit(5, 3)
    b_arrived(6)
    for q in range(4):
        b_unit(6, q)
    finish()
    bx(7)
    with jax.named_scope("c_norm"):
        layer_norm(4)
    with jax.named_scope("c_tiles"):
        last = pieces(col, 0, 8) + pieces(other, 0, 7)
        unit(early, tokens - early, last[:8])
        unit(early, tokens - early, last[8:])
        finish()
    b_arrived(7)
    with jax.named_scope("d_tile"):
        def write(rows, value):
            ys[rows, :] = value.astype(jnp.bfloat16)

        for q in range(4):
            unit(q * (tokens // 4), tokens // 4, pieces(other, 7, 8), write)
        finish()

    with jax.named_scope("sent"):
        wait(w1s.at[pl.ds(0, 14)], send_sem.at[S_W1])
        wait(w2s.at[pl.ds(0, 12)], send_sem.at[S_W2])
        wait(xs.at[0], send_sem.at[S_X])
        wait(gs.at[0], send_sem.at[S_G])


def solution(mesh):
    act_spec = P(None, ("dp", "row"), "col")

    def per_device(x_blk, gamma_blk, w_in_blk, w_out_blk):
        feats = x_blk.shape[2]
        tokens = x_blk.shape[0] * x_blk.shape[1]
        d_model = 2 * feats
        n_pieces = 2 * w_in_blk.shape[1] // PC
        ins = (x_blk.reshape(tokens, feats), gamma_blk.reshape(1, feats), w_in_blk, w_out_blk)
        y = pl.pallas_call(
            kernel,
            name="mlp",
            out_shape=jax.ShapeDtypeStruct((tokens, feats), jnp.bfloat16),
            in_specs=[pl.BlockSpec(memory_space=pltpu.HBM)] * 4,
            out_specs=pl.BlockSpec(memory_space=pltpu.VMEM),
            scratch_shapes=[
                pltpu.VMEM((2, tokens, feats), jnp.bfloat16),
                pltpu.VMEM((n_pieces, d_model, PC), jnp.bfloat16),
                pltpu.VMEM((n_pieces, PC, feats), jnp.bfloat16),
                pltpu.VMEM((tokens, d_model), jnp.bfloat16),
                pltpu.VMEM((tokens, feats), jnp.float32),
                pltpu.VMEM((2, 1, feats), jnp.float32),
                pltpu.SemaphoreType.DMA((10,)),
                pltpu.SemaphoreType.DMA((4,)),
                pltpu.SemaphoreType.DMA((N_RECV,)),
            ],
            compiler_params=pltpu.CompilerParams(collective_id=0, has_side_effects=True, vmem_limit_bytes=52000000),
        )(*[pltpu.with_memory_space_constraint(a, pltpu.HBM) for a in ins])
        return y.reshape(x_blk.shape)

    return jax.shard_map(per_device, mesh=mesh, in_specs=(act_spec, P("col"), P("row", "col"), P("row", "col")), out_specs=act_spec, check_vma=False)
```

```python
import jax
import jax.numpy as jnp
from jax import lax
from jax.experimental import pallas as pl
from jax.experimental.pallas import tpu as pltpu
from jax.sharding import PartitionSpec as P

LN_EPS = 1e-5
MESH = pl.DeviceIdType.MESH
PC = 256
SQRT_2_OVER_PI = 0.7978845608028654
X_ROWS = ((0, 512), (512, 512), (1024, 512), (1536, 320), (1856, 192))

A_ICI, A_D2D, B_Y, B_X, B_D2D, X_Y, G_Y = 0, 4, 8, 24, 32, 40, 45
N_RECV = 46
S_W1, S_W2, S_X, S_G = 0, 1, 2, 3


def gelu(u):
    inner = u * (SQRT_2_OVER_PI + (SQRT_2_OVER_PI * 0.044715) * (u * u))
    return ((0.5 * u) * (1.0 + jnp.tanh(inner))).astype(jnp.bfloat16)


def kernel(x_hbm, g_hbm, w1_hbm, w2_hbm, ys, xs, w1s, w2s, zs, acc, gs, load_sem, send_sem, recv_sem):
    rows1 = w1_hbm.shape[0]
    tokens, d_model = zs.shape
    half_d = d_model // 2

    col = lax.axis_index("col")
    row = lax.axis_index("row")
    core = row % 2
    row_p = row + 1 - 2 * core
    row_x = (row + 2) % 4
    row_xp = (row_p + 2) % 4
    other = 1 - col
    partner, x_nbr, y_nbr = {"row": row_p}, {"row": row_x}, {"col": other}

    def w1p(half, e, r, n=1):
        return w1s.at[pl.ds(half * 8 + e, n), pl.ds(pl.multiple_of(r * rows1, rows1), rows1)]

    def w2p(r, j):
        return w2s.at[(r // 2) * 8 + 2 * j + r % 2]

    def send(ref, dev, s_sem, r_sem):
        pltpu.make_async_remote_copy(
            src_ref=ref, dst_ref=ref, send_sem=send_sem.at[s_sem], recv_sem=recv_sem.at[r_sem],
            device_id=dev, device_id_type=MESH).start()

    def wait(ref, sem):
        pltpu.make_async_copy(ref, ref, sem).wait()

    def load_w(s):
        for e in (2 * s, 2 * s + 1):
            cols = pl.ds((e % 2) * (4 * PC) + (e // 2) * PC, PC)
            dst = w1s.at[col * 8 + e, pl.ds(pl.multiple_of(row * rows1, rows1), rows1)]
            pltpu.make_async_copy(w1_hbm.at[:, cols], dst, load_sem.at[s]).start()
        pltpu.make_async_copy(w2_hbm.at[pl.ds(s * PC, PC)], w2p(row, s), load_sem.at[s]).start()

    def x_part(h, i):
        r0, n = X_ROWS[i]
        return xs.at[h, pl.ds(r0, n)]

    def load_x(i):
        r0, n = X_ROWS[i]
        pltpu.make_async_copy(x_hbm.at[pl.ds(r0, n)], x_part(col, i), load_sem.at[4 + i]).start()

    pltpu.make_async_copy(g_hbm, gs.at[col], load_sem.at[9]).start()
    for s in range(4):
        load_w(s)
        load_x(s)
    load_x(4)

    barrier = pltpu.get_barrier_semaphore()
    for dev in (partner, x_nbr, y_nbr):
        pl.semaphore_signal(barrier, inc=1, device_id=dev, device_id_type=MESH)
    pl.semaphore_wait(barrier, 3)

    def send_x(i):
        wait(x_part(col, i), load_sem.at[4 + i])
        send(x_part(col, i), y_nbr, S_X, X_Y + i)

    def issue(s):
        wait(w1s.at[0], load_sem.at[s])
        w1, w2 = w1p(col, 2 * s, row, 2), w2p(row, s)
        send(w1, x_nbr, S_W1, A_ICI + s)
        send(w2, x_nbr, S_W2, A_ICI + s)
        send(w1, partner, S_W1, A_D2D + s)
        send(w2, partner, S_W2, A_D2D + s)
        send_x(s)

    def relay_a(s):
        wait(w1s.at[0], recv_sem.at[A_ICI + s])
        send(w1p(col, 2 * s, row_x, 2), partner, S_W1, A_D2D + s)
        send(w2p(row_x, s), partner, S_W2, A_D2D + s)

    def half_piece(half, e, h):
        return w1s.at[half * 8 + e, pl.ds(pl.multiple_of(row * rows1 + h * (rows1 // 2), rows1 // 2), rows1 // 2)]

    def relay_by(e, h):
        part = half_piece(other, e, h)
        wait(part, recv_sem.at[B_Y + 2 * e + h])
        send(part, x_nbr, S_W1, B_X + e)
        send(part, partner, S_W1, B_D2D + e)

    def relay_bx(e):
        wait(w1p(other, e, row_x), recv_sem.at[B_X + e])
        send(w1p(other, e, row_x), partner, S_W1, B_D2D + e)

    def layer_norm(i):
        r0, n = X_ROWS[i]
        rb = 64
        wait(x_part(other, i), recv_sem.at[X_Y + i])

        def step(t, _):
            rows = pl.ds(pl.multiple_of(r0 + t * rb, rb), rb)
            parts = [xs[h, rows, :].astype(jnp.float32) for h in range(2)]
            mean = sum(jnp.sum(v, axis=-1, keepdims=True) for v in parts) / d_model
            var = sum(jnp.sum(v * v, axis=-1, keepdims=True) for v in parts) / d_model - mean * mean
            inv = lax.rsqrt(var + LN_EPS)
            for h in range(2):
                zs[rows, h * half_d:(h + 1) * half_d] = ((parts[h] - mean) * inv * gs[h]).astype(jnp.bfloat16)
            acc[rows, :] = xs[col, rows, :].astype(jnp.float32)
            return 0

        lax.fori_loop(0, n // rb, step, 0, unroll=n <= 192)

    held = []

    def finish():
        if held:
            r0, n, ps, hs, store = held.pop()
            rows = pl.ds(r0, n)
            out = None
            for p, h in zip(ps, hs):
                term = jnp.dot(h, w2s[p], preferred_element_type=jnp.float32)
                out = term if out is None else out + term
            if store is None:
                acc[rows, :] += out
            else:
                store(rows, acc[rows, :] + out)

    def unit(r0, n, ps, store=None):
        z = zs[pl.ds(r0, n), :]
        hs = [gelu(jnp.dot(z, w1s[p], preferred_element_type=jnp.float32)) for p in ps]
        finish()
        held.append((r0, n, ps, hs, store))

    def pieces(half, lo, hi):
        return [half * 8 + e for e in range(lo, hi)]

    with jax.named_scope("issue"):
        wait(gs.at[col], load_sem.at[9])
        send(gs.at[col], y_nbr, S_G, G_Y)
        issue(0)
        issue(1)
        wait(gs.at[other], recv_sem.at[G_Y])
    for s in range(3):
        with jax.named_scope(f"a_wait_x{s}"):
            if s < 2:
                issue(s + 2)
            if s == 1:
                for e in range(8):
                    for h in range(2):
                        send(half_piece(col, e, h), y_nbr, S_W1, B_Y + 2 * e + h)
                send_x(4)
            relay_a(s)
        with jax.named_scope(f"a_norm{s}"):
            layer_norm(s)
        with jax.named_scope(f"a_wait_d{s}"):
            wait(w1s.at[pl.ds(0, 2)], recv_sem.at[A_D2D + s])
        with jax.named_scope(f"a_tiles{s}"):
            def a_tile(t, _):
                q = t // (s + 1)
                g, j = t - q * (t - s), s - q * (t - s)
                p = col * 8 + 2 * j
                for k in (0, 256):
                    unit(pl.multiple_of(g * 512 + k, 256), 256, (p, p + 1))
                finish()
                return 0

            lax.fori_loop(0, 2 * s + 1, a_tile, 0)

    early = X_ROWS[4][0]
    third = early // 3
    with jax.named_scope("a_norm3"):
        layer_norm(3)
    quarter = early // 4

    def first(e):
        with jax.named_scope(f"first{e}"):
            unit(*X_ROWS[3], pieces(col, 2 * e, 2 * e + 2))

    def a_unit(q):
        unit(q * quarter, quarter, pieces(col, 6, 8))

    def b_unit(e, q):
        unit(q * quarter, quarter, pieces(other, e, e + 1))

    def by(e, h):
        with jax.named_scope(f"by{e}{h}"):
            relay_by(e, h)

    def bx(e):
        with jax.named_scope(f"bx{e}"):
            relay_bx(e)

    def b_arrived(e):
        with jax.named_scope(f"bd{e}"):
            wait(w2s.at[0], recv_sem.at[B_D2D + e])

    first(0)
    by(0, 0)
    first(1)
    first(2)
    by(0, 1)
    with jax.named_scope("a3"):
        relay_a(3)
    by(1, 0)
    with jax.named_scope("ad3"):
        wait(w1s.at[pl.ds(0, 2)], recv_sem.at[A_D2D + 3])
    a_unit(0)
    by(1, 1)
    a_unit(1)
    a_unit(2)
    bx(0)
    by(2, 0)
    a_unit(3)
    for e in range(5):
        by(e + 2, 1)
        b_arrived(e)
        b_unit(e, 0)
        b_unit(e, 1)
        bx(e + 1)
        by(e + 3, 0)
        b_unit(e, 2)
        b_unit(e, 3)
    by(7, 1)
    b_arrived(5)
    b_unit(5, 0)
    b_unit(5, 1)
    bx(6)
    b_unit(5, 2)
    b_unit(5, 3)
    b_arrived(6)
    for q in range(4):
        b_unit(6, q)
    finish()
    bx(7)
    with jax.named_scope("c_norm"):
        layer_norm(4)
    with jax.named_scope("c_tiles"):
        last = pieces(col, 0, 8) + pieces(other, 0, 7)
        for ps in (last[:8], last[8:]):
            @pl.when(row >= 0)
            def _():
                unit(early, tokens - early, ps)
                finish()
    b_arrived(7)
    with jax.named_scope("d_tile"):
        def write(rows, value):
            ys[rows, :] = value.astype(jnp.bfloat16)

        for q in range(4):
            unit(q * (tokens // 4), tokens // 4, pieces(other, 7, 8), write)
        finish()

    with jax.named_scope("sent"):
        wait(w1s.at[pl.ds(0, 14)], send_sem.at[S_W1])
        wait(w2s.at[pl.ds(0, 12)], send_sem.at[S_W2])
        wait(xs.at[0], send_sem.at[S_X])
        wait(gs.at[0], send_sem.at[S_G])


def solution(mesh):
    act_spec = P(None, ("dp", "row"), "col")

    def per_device(x_blk, gamma_blk, w_in_blk, w_out_blk):
        feats = x_blk.shape[2]
        tokens = x_blk.shape[0] * x_blk.shape[1]
        d_model = 2 * feats
        n_pieces = 2 * w_in_blk.shape[1] // PC
        ins = (x_blk.reshape(tokens, feats), gamma_blk.reshape(1, feats), w_in_blk, w_out_blk)
        y = pl.pallas_call(
            kernel,
            name="mlp",
            out_shape=jax.ShapeDtypeStruct((tokens, feats), jnp.bfloat16),
            in_specs=[pl.BlockSpec(memory_space=pltpu.HBM)] * 4,
            out_specs=pl.BlockSpec(memory_space=pltpu.VMEM),
            scratch_shapes=[
                pltpu.VMEM((2, tokens, feats), jnp.bfloat16),
                pltpu.VMEM((n_pieces, d_model, PC), jnp.bfloat16),
                pltpu.VMEM((n_pieces, PC, feats), jnp.bfloat16),
                pltpu.VMEM((tokens, d_model), jnp.bfloat16),
                pltpu.VMEM((tokens, feats), jnp.float32),
                pltpu.VMEM((2, 1, feats), jnp.float32),
                pltpu.SemaphoreType.DMA((10,)),
                pltpu.SemaphoreType.DMA((4,)),
                pltpu.SemaphoreType.DMA((N_RECV,)),
            ],
            compiler_params=pltpu.CompilerParams(collective_id=0, has_side_effects=True, vmem_limit_bytes=52000000),
        )(*[pltpu.with_memory_space_constraint(a, pltpu.HBM) for a in ins])
        return y.reshape(x_blk.shape)

    return jax.shard_map(per_device, mesh=mesh, in_specs=(act_spec, P("col"), P("row", "col"), P("row", "col")), out_specs=act_spec, check_vma=False)
```

```python
import jax
import jax.numpy as jnp
from jax import lax
from jax.experimental import pallas as pl
from jax.experimental.pallas import tpu as pltpu
from jax.sharding import PartitionSpec as P

LN_EPS = 1e-5
MESH = pl.DeviceIdType.MESH
PC = 256
SQRT_2_OVER_PI = 0.7978845608028654
X_ROWS = ((0, 512), (512, 512), (1024, 512), (1536, 320), (1856, 192))

A_ICI, A_D2D, B_Y, B_X, B_D2D, X_Y, G_Y = 0, 4, 8, 24, 32, 40, 45
N_RECV = 46
S_W1, S_W2, S_X, S_G = 0, 1, 2, 3


def gelu(u):
    inner = u * (SQRT_2_OVER_PI + (SQRT_2_OVER_PI * 0.044715) * (u * u))
    return ((0.5 * u) * (1.0 + jnp.tanh(inner))).astype(jnp.bfloat16)


def kernel(x_hbm, g_hbm, w1_hbm, w2_hbm, ys, xs, w1s, w2s, zs, acc, gs, load_sem, send_sem, recv_sem):
    rows1 = w1_hbm.shape[0]
    tokens, d_model = zs.shape
    half_d = d_model // 2

    col = lax.axis_index("col")
    row = lax.axis_index("row")
    core = row % 2
    row_p = row + 1 - 2 * core
    row_x = (row + 2) % 4
    row_xp = (row_p + 2) % 4
    other = 1 - col
    partner, x_nbr, y_nbr = {"row": row_p}, {"row": row_x}, {"col": other}

    def w1p(half, e, r, n=1):
        return w1s.at[pl.ds(half * 8 + e, n), pl.ds(pl.multiple_of(r * rows1, rows1), rows1)]

    def w2p(r, j):
        return w2s.at[(r // 2) * 8 + 2 * j + r % 2]

    def send(ref, dev, s_sem, r_sem):
        pltpu.make_async_remote_copy(
            src_ref=ref, dst_ref=ref, send_sem=send_sem.at[s_sem], recv_sem=recv_sem.at[r_sem],
            device_id=dev, device_id_type=MESH).start()

    def wait(ref, sem):
        pltpu.make_async_copy(ref, ref, sem).wait()

    def load_w(s):
        for e in (2 * s, 2 * s + 1):
            cols = pl.ds((e % 2) * (4 * PC) + (e // 2) * PC, PC)
            dst = w1s.at[col * 8 + e, pl.ds(pl.multiple_of(row * rows1, rows1), rows1)]
            pltpu.make_async_copy(w1_hbm.at[:, cols], dst, load_sem.at[s]).start()
        pltpu.make_async_copy(w2_hbm.at[pl.ds(s * PC, PC)], w2p(row, s), load_sem.at[s]).start()

    def x_part(h, i):
        r0, n = X_ROWS[i]
        return xs.at[h, pl.ds(r0, n)]

    def load_x(i):
        r0, n = X_ROWS[i]
        pltpu.make_async_copy(x_hbm.at[pl.ds(r0, n)], x_part(col, i), load_sem.at[4 + i]).start()

    pltpu.make_async_copy(g_hbm, gs.at[col], load_sem.at[9]).start()
    for s in range(4):
        load_w(s)
        load_x(s)
    load_x(4)

    barrier = pltpu.get_barrier_semaphore()
    for dev in (partner, x_nbr, y_nbr):
        pl.semaphore_signal(barrier, inc=1, device_id=dev, device_id_type=MESH)
    pl.semaphore_wait(barrier, 3)

    def send_x(i):
        wait(x_part(col, i), load_sem.at[4 + i])
        send(x_part(col, i), y_nbr, S_X, X_Y + i)

    def issue(s):
        wait(w1s.at[0], load_sem.at[s])
        w1, w2 = w1p(col, 2 * s, row, 2), w2p(row, s)
        send(w1, x_nbr, S_W1, A_ICI + s)
        send(w2, x_nbr, S_W2, A_ICI + s)
        send(w1, partner, S_W1, A_D2D + s)
        send(w2, partner, S_W2, A_D2D + s)
        send_x(s)

    def relay_a(s):
        wait(w1s.at[0], recv_sem.at[A_ICI + s])
        send(w1p(col, 2 * s, row_x, 2), partner, S_W1, A_D2D + s)
        send(w2p(row_x, s), partner, S_W2, A_D2D + s)

    def half_piece(half, e, h):
        return w1s.at[half * 8 + e, pl.ds(pl.multiple_of(row * rows1 + h * (rows1 // 2), rows1 // 2), rows1 // 2)]

    def relay_by(e, h):
        part = half_piece(other, e, h)
        wait(part, recv_sem.at[B_Y + 2 * e + h])
        send(part, x_nbr, S_W1, B_X + e)
        send(part, partner, S_W1, B_D2D + e)

    def relay_bx(e):
        wait(w1p(other, e, row_x), recv_sem.at[B_X + e])
        send(w1p(other, e, row_x), partner, S_W1, B_D2D + e)

    def layer_norm(i):
        r0, n = X_ROWS[i]
        rb = 64
        wait(x_part(other, i), recv_sem.at[X_Y + i])

        def step(t, _):
            rows = pl.ds(pl.multiple_of(r0 + t * rb, rb), rb)
            parts = [xs[h, rows, :].astype(jnp.float32) for h in range(2)]
            mean = sum(jnp.sum(v, axis=-1, keepdims=True) for v in parts) / d_model
            var = sum(jnp.sum(v * v, axis=-1, keepdims=True) for v in parts) / d_model - mean * mean
            inv = lax.rsqrt(var + LN_EPS)
            for h in range(2):
                zs[rows, h * half_d:(h + 1) * half_d] = ((parts[h] - mean) * inv * gs[h]).astype(jnp.bfloat16)
            acc[rows, :] = xs[col, rows, :].astype(jnp.float32)
            return 0

        lax.fori_loop(0, n // rb, step, 0, unroll=n <= 192)

    held = []

    def finish():
        if held:
            r0, n, ps, hs, store = held.pop()
            rows = pl.ds(r0, n)
            out = None
            for p, h in zip(ps, hs):
                term = jnp.dot(h, w2s[p], preferred_element_type=jnp.float32)
                out = term if out is None else out + term
            if store is None:
                acc[rows, :] += out
            else:
                store(rows, acc[rows, :] + out)

    def unit(r0, n, ps, store=None):
        z = zs[pl.ds(r0, n), :]
        hs = [gelu(jnp.dot(z, w1s[p], preferred_element_type=jnp.float32)) for p in ps]
        finish()
        held.append((r0, n, ps, hs, store))

    def pieces(half, lo, hi):
        return [half * 8 + e for e in range(lo, hi)]

    with jax.named_scope("issue"):
        wait(gs.at[col], load_sem.at[9])
        send(gs.at[col], y_nbr, S_G, G_Y)
        issue(0)
        issue(1)
        wait(gs.at[other], recv_sem.at[G_Y])
    for s in range(3):
        with jax.named_scope(f"a_wait_x{s}"):
            if s < 2:
                issue(s + 2)
            if s == 1:
                for e in range(8):
                    for h in range(2):
                        send(half_piece(col, e, h), y_nbr, S_W1, B_Y + 2 * e + h)
                send_x(4)
            relay_a(s)
        with jax.named_scope(f"a_norm{s}"):
            layer_norm(s)
        with jax.named_scope(f"a_wait_d{s}"):
            wait(w1s.at[pl.ds(0, 2)], recv_sem.at[A_D2D + s])
        with jax.named_scope(f"a_tiles{s}"):
            def a_tile(t, _):
                q = t // (s + 1)
                g, j = t - q * (t - s), s - q * (t - s)
                p = col * 8 + 2 * j
                for k in (0, 256):
                    unit(pl.multiple_of(g * 512 + k, 256), 256, (p, p + 1))
                finish()
                return 0

            lax.fori_loop(0, 2 * s + 1, a_tile, 0)

    early = X_ROWS[4][0]
    third = early // 3
    with jax.named_scope("a_norm3"):
        layer_norm(3)
    quarter = early // 4

    def first(e):
        with jax.named_scope(f"first{e}"):
            unit(*X_ROWS[3], pieces(col, 2 * e, 2 * e + 2))

    def a_unit(q):
        unit(q * quarter, quarter, pieces(col, 6, 8))

    def b_unit(e, q):
        unit(q * quarter, quarter, pieces(other, e, e + 1))

    def by(e, h):
        with jax.named_scope(f"by{e}{h}"):
            relay_by(e, h)

    def bx(e):
        with jax.named_scope(f"bx{e}"):
            relay_bx(e)

    def b_arrived(e):
        with jax.named_scope(f"bd{e}"):
            wait(w2s.at[0], recv_sem.at[B_D2D + e])

    first(0)
    by(0, 0)
    first(1)
    first(2)
    by(0, 1)
    with jax.named_scope("a3"):
        relay_a(3)
    by(1, 0)
    with jax.named_scope("ad3"):
        wait(w1s.at[pl.ds(0, 2)], recv_sem.at[A_D2D + 3])
    a_unit(0)
    by(1, 1)
    a_unit(1)
    a_unit(2)
    bx(0)
    by(2, 0)
    a_unit(3)
    for e in range(5):
        by(e + 2, 1)
        b_arrived(e)
        b_unit(e, 0)
        b_unit(e, 1)
        bx(e + 1)
        by(e + 3, 0)
        b_unit(e, 2)
        b_unit(e, 3)
    by(7, 1)
    b_arrived(5)
    b_unit(5, 0)
    b_unit(5, 1)
    bx(6)
    b_unit(5, 2)
    b_unit(5, 3)
    b_arrived(6)
    for q in range(4):
        b_unit(6, q)
    finish()
    bx(7)
    with jax.named_scope("c_norm"):
        layer_norm(4)
    with jax.named_scope("c_tiles"):
        last = pieces(col, 0, 8) + pieces(other, 0, 7)
        @pl.when(row >= 0)
        def _():
            unit(early, tokens - early, last)
            finish()
    b_arrived(7)
    with jax.named_scope("d_tile"):
        def write(rows, value):
            ys[rows, :] = value.astype(jnp.bfloat16)

        r0 = 0
        for n in (512, 512, 512, 384, 128):
            unit(r0, n, pieces(other, 7, 8), write)
            r0 += n
        finish()

    with jax.named_scope("sent"):
        wait(w1s.at[pl.ds(0, 14)], send_sem.at[S_W1])
        wait(w2s.at[pl.ds(0, 12)], send_sem.at[S_W2])
        wait(xs.at[0], send_sem.at[S_X])
        wait(gs.at[0], send_sem.at[S_G])


def solution(mesh):
    act_spec = P(None, ("dp", "row"), "col")

    def per_device(x_blk, gamma_blk, w_in_blk, w_out_blk):
        feats = x_blk.shape[2]
        tokens = x_blk.shape[0] * x_blk.shape[1]
        d_model = 2 * feats
        n_pieces = 2 * w_in_blk.shape[1] // PC
        ins = (x_blk.reshape(tokens, feats), gamma_blk.reshape(1, feats), w_in_blk, w_out_blk)
        y = pl.pallas_call(
            kernel,
            name="mlp",
            out_shape=jax.ShapeDtypeStruct((tokens, feats), jnp.bfloat16),
            in_specs=[pl.BlockSpec(memory_space=pltpu.HBM)] * 4,
            out_specs=pl.BlockSpec(memory_space=pltpu.VMEM),
            scratch_shapes=[
                pltpu.VMEM((2, tokens, feats), jnp.bfloat16),
                pltpu.VMEM((n_pieces, d_model, PC), jnp.bfloat16),
                pltpu.VMEM((n_pieces, PC, feats), jnp.bfloat16),
                pltpu.VMEM((tokens, d_model), jnp.bfloat16),
                pltpu.VMEM((tokens, feats), jnp.float32),
                pltpu.VMEM((2, 1, feats), jnp.float32),
                pltpu.SemaphoreType.DMA((10,)),
                pltpu.SemaphoreType.DMA((4,)),
                pltpu.SemaphoreType.DMA((N_RECV,)),
            ],
            compiler_params=pltpu.CompilerParams(collective_id=0, has_side_effects=True, vmem_limit_bytes=52000000),
        )(*[pltpu.with_memory_space_constraint(a, pltpu.HBM) for a in ins])
        return y.reshape(x_blk.shape)

    return jax.shard_map(per_device, mesh=mesh, in_specs=(act_spec, P("col"), P("row", "col"), P("row", "col")), out_specs=act_spec, check_vma=False)
```

```python
import jax
import jax.numpy as jnp
from jax import lax
from jax.experimental import pallas as pl
from jax.experimental.pallas import tpu as pltpu
from jax.sharding import PartitionSpec as P

LN_EPS = 1e-5
MESH = pl.DeviceIdType.MESH
PC = 256
SQRT_2_OVER_PI = 0.7978845608028654
X_ROWS = ((0, 512), (512, 512), (1024, 512), (1536, 320), (1856, 192))

A_ICI, A_D2D, B_Y, B_X, B_D2D, X_Y, G_Y = 0, 4, 8, 25, 33, 41, 46
N_RECV = 47
S_W1, S_W2, S_X, S_G = 0, 1, 2, 3


def gelu(u):
    inner = u * (SQRT_2_OVER_PI + (SQRT_2_OVER_PI * 0.044715) * (u * u))
    return ((0.5 * u) * (1.0 + jnp.tanh(inner))).astype(jnp.bfloat16)


def kernel(x_hbm, g_hbm, w1_hbm, w2_hbm, ys, xs, w1s, w2s, zs, acc, gs, load_sem, send_sem, recv_sem):
    rows1 = w1_hbm.shape[0]
    tokens, d_model = zs.shape
    half_d = d_model // 2

    col = lax.axis_index("col")
    row = lax.axis_index("row")
    core = row % 2
    row_p = row + 1 - 2 * core
    row_x = (row + 2) % 4
    row_xp = (row_p + 2) % 4
    other = 1 - col
    partner, x_nbr, y_nbr = {"row": row_p}, {"row": row_x}, {"col": other}

    def w1p(half, e, r, n=1):
        return w1s.at[pl.ds(half * 8 + e, n), pl.ds(pl.multiple_of(r * rows1, rows1), rows1)]

    def w2p(r, j):
        return w2s.at[(r // 2) * 8 + 2 * j + r % 2]

    def send(ref, dev, s_sem, r_sem):
        pltpu.make_async_remote_copy(
            src_ref=ref, dst_ref=ref, send_sem=send_sem.at[s_sem], recv_sem=recv_sem.at[r_sem],
            device_id=dev, device_id_type=MESH).start()

    def wait(ref, sem):
        pltpu.make_async_copy(ref, ref, sem).wait()

    def load_w(s):
        for e in (2 * s, 2 * s + 1):
            cols = pl.ds((e % 2) * (4 * PC) + (e // 2) * PC, PC)
            dst = w1s.at[col * 8 + e, pl.ds(pl.multiple_of(row * rows1, rows1), rows1)]
            pltpu.make_async_copy(w1_hbm.at[:, cols], dst, load_sem.at[s]).start()
        pltpu.make_async_copy(w2_hbm.at[pl.ds(s * PC, PC)], w2p(row, s), load_sem.at[s]).start()

    def x_part(h, i):
        r0, n = X_ROWS[i]
        return xs.at[h, pl.ds(r0, n)]

    def load_x(i):
        r0, n = X_ROWS[i]
        pltpu.make_async_copy(x_hbm.at[pl.ds(r0, n)], x_part(col, i), load_sem.at[4 + i]).start()

    pltpu.make_async_copy(g_hbm, gs.at[col], load_sem.at[9]).start()
    for s in range(4):
        load_w(s)
        load_x(s)
    load_x(4)

    barrier = pltpu.get_barrier_semaphore()
    for dev in (partner, x_nbr, y_nbr):
        pl.semaphore_signal(barrier, inc=1, device_id=dev, device_id_type=MESH)
    pl.semaphore_wait(barrier, 3)

    def send_x(i):
        wait(x_part(col, i), load_sem.at[4 + i])
        send(x_part(col, i), y_nbr, S_X, X_Y + i)

    def issue(s):
        wait(w1s.at[0], load_sem.at[s])
        w1, w2 = w1p(col, 2 * s, row, 2), w2p(row, s)
        send(w1, x_nbr, S_W1, A_ICI + s)
        send(w2, x_nbr, S_W2, A_ICI + s)
        send(w1, partner, S_W1, A_D2D + s)
        send(w2, partner, S_W2, A_D2D + s)
        send_x(s)

    def relay_a(s):
        wait(w1s.at[0], recv_sem.at[A_ICI + s])
        send(w1p(col, 2 * s, row_x, 2), partner, S_W1, A_D2D + s)
        send(w2p(row_x, s), partner, S_W2, A_D2D + s)

    def part(half, e, h):
        lo, n = ((0, 2), (2, 2))[h] if e != 6 else ((0, 2), (2, 1), (3, 1))[h]
        q = rows1 // 4
        return w1s.at[half * 8 + e, pl.ds(pl.multiple_of(row * rows1 + lo * q, q), n * q)]

    def part_sem(e, h):
        return B_Y + 2 * e + h + (e > 6)

    def relay_by(e, h):
        rows = part(other, e, h)
        wait(rows, recv_sem.at[part_sem(e, h)])
        send(rows, x_nbr, S_W1, B_X + e)
        send(rows, partner, S_W1, B_D2D + e)

    def relay_bx(e):
        wait(w1p(other, e, row_x), recv_sem.at[B_X + e])
        send(w1p(other, e, row_x), partner, S_W1, B_D2D + e)

    def layer_norm(i):
        r0, n = X_ROWS[i]
        rb = 64
        wait(x_part(other, i), recv_sem.at[X_Y + i])

        def step(t, _):
            rows = pl.ds(pl.multiple_of(r0 + t * rb, rb), rb)
            parts = [xs[h, rows, :].astype(jnp.float32) for h in range(2)]
            mean = sum(jnp.sum(v, axis=-1, keepdims=True) for v in parts) / d_model
            var = sum(jnp.sum(v * v, axis=-1, keepdims=True) for v in parts) / d_model - mean * mean
            inv = lax.rsqrt(var + LN_EPS)
            for h in range(2):
                zs[rows, h * half_d:(h + 1) * half_d] = ((parts[h] - mean) * inv * gs[h]).astype(jnp.bfloat16)
            acc[rows, :] = xs[col, rows, :].astype(jnp.float32)
            return 0

        lax.fori_loop(0, n // rb, step, 0, unroll=n <= 192)

    held = []

    def finish():
        if held:
            r0, n, ps, hs, store = held.pop()
            rows = pl.ds(r0, n)
            out = None
            for p, h in zip(ps, hs):
                term = jnp.dot(h, w2s[p], preferred_element_type=jnp.float32)
                out = term if out is None else out + term
            if store is None:
                acc[rows, :] += out
            else:
                store(rows, acc[rows, :] + out)

    def unit(r0, n, ps, store=None):
        z = zs[pl.ds(r0, n), :]
        hs = [gelu(jnp.dot(z, w1s[p], preferred_element_type=jnp.float32)) for p in ps]
        finish()
        held.append((r0, n, ps, hs, store))

    def pieces(half, lo, hi):
        return [half * 8 + e for e in range(lo, hi)]

    with jax.named_scope("issue"):
        wait(gs.at[col], load_sem.at[9])
        send(gs.at[col], y_nbr, S_G, G_Y)
        issue(0)
        issue(1)
        wait(gs.at[other], recv_sem.at[G_Y])
    for s in range(3):
        with jax.named_scope(f"a_wait_x{s}"):
            if s < 2:
                issue(s + 2)
            if s == 1:
                for e in range(8):
                    for h in range(2 + (e == 6)):
                        send(part(col, e, h), y_nbr, S_W1, part_sem(e, h))
                send_x(4)
            relay_a(s)
        with jax.named_scope(f"a_norm{s}"):
            layer_norm(s)
        with jax.named_scope(f"a_wait_d{s}"):
            wait(w1s.at[pl.ds(0, 2)], recv_sem.at[A_D2D + s])
        with jax.named_scope(f"a_tiles{s}"):
            def a_tile(t, _):
                q = t // (s + 1)
                g, j = t - q * (t - s), s - q * (t - s)
                p = col * 8 + 2 * j
                for k in (0, 256):
                    unit(pl.multiple_of(g * 512 + k, 256), 256, (p, p + 1))
                finish()
                return 0

            lax.fori_loop(0, 2 * s + 1, a_tile, 0)

    early = X_ROWS[4][0]
    third = early // 3
    with jax.named_scope("a_norm3"):
        layer_norm(3)
    quarter = early // 4

    def first(e):
        with jax.named_scope(f"first{e}"):
            unit(*X_ROWS[3], pieces(col, 2 * e, 2 * e + 2))

    def a_unit(q):
        unit(q * quarter, quarter, pieces(col, 6, 8))

    def b_unit(e, q):
        unit(q * quarter, quarter, pieces(other, e, e + 1))

    def by(e, h):
        with jax.named_scope(f"by{e}{h}"):
            relay_by(e, h)

    def bx(e):
        with jax.named_scope(f"bx{e}"):
            relay_bx(e)

    def b_arrived(e):
        with jax.named_scope(f"bd{e}"):
            wait(w2s.at[0], recv_sem.at[B_D2D + e])

    first(0)
    by(0, 0)
    first(1)
    first(2)
    by(0, 1)
    with jax.named_scope("a3"):
        relay_a(3)
    by(1, 0)
    with jax.named_scope("ad3"):
        wait(w1s.at[pl.ds(0, 2)], recv_sem.at[A_D2D + 3])
    a_unit(0)
    by(1, 1)
    a_unit(1)
    a_unit(2)
    bx(0)
    by(2, 0)
    a_unit(3)
    for e in range(5):
        by(e + 2, 1 + (e == 4))
        b_arrived(e)
        b_unit(e, 0)
        b_unit(e, 1)
        bx(e + 1)
        by(e + 3, 0)
        b_unit(e, 2)
        if e == 3:
            by(6, 1)
        b_unit(e, 3)
    by(7, 1)
    b_arrived(5)
    b_unit(5, 0)
    b_unit(5, 1)
    bx(6)
    b_unit(5, 2)
    b_unit(5, 3)
    b_arrived(6)
    for q in range(4):
        b_unit(6, q)
    finish()
    bx(7)
    with jax.named_scope("c_norm"):
        layer_norm(4)
    with jax.named_scope("c_tiles"):
        last = pieces(col, 0, 8) + pieces(other, 0, 7)
        for ps in (last[:8], last[8:]):
            @pl.when(row >= 0)
            def _():
                unit(early, tokens - early, ps)
                finish()
    b_arrived(7)
    with jax.named_scope("d_tile"):
        def write(rows, value):
            ys[rows, :] = value.astype(jnp.bfloat16)

        for q in range(4):
            unit(q * (tokens // 4), tokens // 4, pieces(other, 7, 8), write)
        finish()

    with jax.named_scope("sent"):
        wait(w1s.at[pl.ds(0, 14)], send_sem.at[S_W1])
        wait(w2s.at[pl.ds(0, 12)], send_sem.at[S_W2])
        wait(xs.at[0], send_sem.at[S_X])
        wait(gs.at[0], send_sem.at[S_G])


def solution(mesh):
    act_spec = P(None, ("dp", "row"), "col")

    def per_device(x_blk, gamma_blk, w_in_blk, w_out_blk):
        feats = x_blk.shape[2]
        tokens = x_blk.shape[0] * x_blk.shape[1]
        d_model = 2 * feats
        n_pieces = 2 * w_in_blk.shape[1] // PC
        ins = (x_blk.reshape(tokens, feats), gamma_blk.reshape(1, feats), w_in_blk, w_out_blk)
        y = pl.pallas_call(
            kernel,
            name="mlp",
            out_shape=jax.ShapeDtypeStruct((tokens, feats), jnp.bfloat16),
            in_specs=[pl.BlockSpec(memory_space=pltpu.HBM)] * 4,
            out_specs=pl.BlockSpec(memory_space=pltpu.VMEM),
            scratch_shapes=[
                pltpu.VMEM((2, tokens, feats), jnp.bfloat16),
                pltpu.VMEM((n_pieces, d_model, PC), jnp.bfloat16),
                pltpu.VMEM((n_pieces, PC, feats), jnp.bfloat16),
                pltpu.VMEM((tokens, d_model), jnp.bfloat16),
                pltpu.VMEM((tokens, feats), jnp.float32),
                pltpu.VMEM((2, 1, feats), jnp.float32),
                pltpu.SemaphoreType.DMA((10,)),
                pltpu.SemaphoreType.DMA((4,)),
                pltpu.SemaphoreType.DMA((N_RECV,)),
            ],
            compiler_params=pltpu.CompilerParams(collective_id=0, has_side_effects=True, vmem_limit_bytes=52000000),
        )(*[pltpu.with_memory_space_constraint(a, pltpu.HBM) for a in ins])
        return y.reshape(x_blk.shape)

    return jax.shard_map(per_device, mesh=mesh, in_specs=(act_spec, P("col"), P("row", "col"), P("row", "col")), out_specs=act_spec, check_vma=False)
```

```python
import jax
import jax.numpy as jnp
from jax import lax
from jax.experimental import pallas as pl
from jax.experimental.pallas import tpu as pltpu
from jax.sharding import PartitionSpec as P

LN_EPS = 1e-5
MESH = pl.DeviceIdType.MESH
PC = 256
SQRT_2_OVER_PI = 0.7978845608028654
X_ROWS = ((0, 512), (512, 512), (1024, 512), (1536, 320), (1856, 192))

A_ICI, A_D2D, B_Y, B_X, B_D2D, X_Y, G_Y = 0, 4, 8, 24, 32, 40, 45
N_RECV = 46
S_W1, S_W2, S_X, S_G = 0, 1, 2, 3


def gelu(u):
    inner = u * (SQRT_2_OVER_PI + (SQRT_2_OVER_PI * 0.044715) * (u * u))
    return ((0.5 * u) * (1.0 + jnp.tanh(inner))).astype(jnp.bfloat16)


def kernel(x_hbm, g_hbm, w1_hbm, w2_hbm, ys, xs, w1s, w2s, zs, acc, gs, load_sem, send_sem, recv_sem):
    rows1 = w1_hbm.shape[0]
    tokens, d_model = zs.shape
    half_d = d_model // 2

    col = lax.axis_index("col")
    row = lax.axis_index("row")
    core = row % 2
    row_p = row + 1 - 2 * core
    row_x = (row + 2) % 4
    row_xp = (row_p + 2) % 4
    other = 1 - col
    partner, x_nbr, y_nbr = {"row": row_p}, {"row": row_x}, {"col": other}

    def w1p(half, e, r, n=1):
        return w1s.at[pl.ds(half * 8 + e, n), pl.ds(pl.multiple_of(r * rows1, rows1), rows1)]

    def w2p(r, j):
        return w2s.at[(r // 2) * 8 + 2 * j + r % 2]

    def send(ref, dev, s_sem, r_sem):
        pltpu.make_async_remote_copy(
            src_ref=ref, dst_ref=ref, send_sem=send_sem.at[s_sem], recv_sem=recv_sem.at[r_sem],
            device_id=dev, device_id_type=MESH).start()

    def wait(ref, sem):
        pltpu.make_async_copy(ref, ref, sem).wait()

    def load_w(s):
        for e in (2 * s, 2 * s + 1):
            cols = pl.ds((e % 2) * (4 * PC) + (e // 2) * PC, PC)
            dst = w1s.at[col * 8 + e, pl.ds(pl.multiple_of(row * rows1, rows1), rows1)]
            pltpu.make_async_copy(w1_hbm.at[:, cols], dst, load_sem.at[0 if s == 0 else 3]).start()
        pltpu.make_async_copy(w2_hbm.at[pl.ds(s * PC, PC)], w2p(row, s), load_sem.at[0 if s == 0 else 3]).start()

    def x_part(h, i):
        r0, n = X_ROWS[i]
        return xs.at[h, pl.ds(r0, n)]

    def load_x(i):
        r0, n = X_ROWS[i]
        pltpu.make_async_copy(x_hbm.at[pl.ds(r0, n)], x_part(col, i), load_sem.at[1 if i == 0 else 3]).start()

    pltpu.make_async_copy(g_hbm, gs.at[col], load_sem.at[2]).start()
    for s in range(4):
        load_w(s)
        load_x(s)
    load_x(4)

    barrier = pltpu.get_barrier_semaphore()
    for dev in (partner, x_nbr, y_nbr):
        pl.semaphore_signal(barrier, inc=1, device_id=dev, device_id_type=MESH)
    pl.semaphore_wait(barrier, 3)

    def send_x(i):
        if i == 0:
            wait(x_part(col, i), load_sem.at[1])
        send(x_part(col, i), y_nbr, S_X, X_Y + i)

    def issue(s):
        if s == 0:
            wait(w1s.at[0], load_sem.at[0])
        elif s == 1:
            wait(w1s.at[pl.ds(0, 6)], load_sem.at[3])
        w1, w2 = w1p(col, 2 * s, row, 2), w2p(row, s)
        send(w1, x_nbr, S_W1, A_ICI + s)
        send(w2, x_nbr, S_W2, A_ICI + s)
        send(w1, partner, S_W1, A_D2D + s)
        send(w2, partner, S_W2, A_D2D + s)
        send_x(s)

    def relay_a(s):
        wait(w1s.at[0], recv_sem.at[A_ICI + s])
        send(w1p(col, 2 * s, row_x, 2), partner, S_W1, A_D2D + s)
        send(w2p(row_x, s), partner, S_W2, A_D2D + s)

    def half_piece(half, e, h):
        return w1s.at[half * 8 + e, pl.ds(pl.multiple_of(row * rows1 + h * (rows1 // 2), rows1 // 2), rows1 // 2)]

    def relay_by(e, h):
        part = half_piece(other, e, h)
        wait(part, recv_sem.at[B_Y + 2 * e + h])
        send(part, x_nbr, S_W1, B_X + e)
        send(part, partner, S_W1, B_D2D + e)

    def relay_bx(e):
        wait(w1p(other, e, row_x), recv_sem.at[B_X + e])
        send(w1p(other, e, row_x), partner, S_W1, B_D2D + e)

    def layer_norm(i):
        r0, n = X_ROWS[i]
        rb = 64
        wait(x_part(other, i), recv_sem.at[X_Y + i])

        def step(t, _):
            rows = pl.ds(pl.multiple_of(r0 + t * rb, rb), rb)
            parts = [xs[h, rows, :].astype(jnp.float32) for h in range(2)]
            mean = sum(jnp.sum(v, axis=-1, keepdims=True) for v in parts) / d_model
            var = sum(jnp.sum(v * v, axis=-1, keepdims=True) for v in parts) / d_model - mean * mean
            inv = lax.rsqrt(var + LN_EPS)
            for h in range(2):
                zs[rows, h * half_d:(h + 1) * half_d] = ((parts[h] - mean) * inv * gs[h]).astype(jnp.bfloat16)
            acc[rows, :] = xs[col, rows, :].astype(jnp.float32)
            return 0

        lax.fori_loop(0, n // rb, step, 0, unroll=n <= 192)

    held = []

    def finish():
        if held:
            r0, n, ps, hs, store = held.pop()
            rows = pl.ds(r0, n)
            out = None
            for p, h in zip(ps, hs):
                term = jnp.dot(h, w2s[p], preferred_element_type=jnp.float32)
                out = term if out is None else out + term
            if store is None:
                acc[rows, :] += out
            else:
                store(rows, acc[rows, :] + out)

    def unit(r0, n, ps, store=None):
        z = zs[pl.ds(r0, n), :]
        hs = [gelu(jnp.dot(z, w1s[p], preferred_element_type=jnp.float32)) for p in ps]
        finish()
        held.append((r0, n, ps, hs, store))

    def pieces(half, lo, hi):
        return [half * 8 + e for e in range(lo, hi)]

    with jax.named_scope("issue"):
        wait(gs.at[col], load_sem.at[2])
        send(gs.at[col], y_nbr, S_G, G_Y)
        issue(0)
        issue(1)
        wait(gs.at[other], recv_sem.at[G_Y])
    for s in range(3):
        with jax.named_scope(f"a_wait_x{s}"):
            if s < 2:
                issue(s + 2)
            if s == 1:
                for e in range(8):
                    for h in range(2):
                        send(half_piece(col, e, h), y_nbr, S_W1, B_Y + 2 * e + h)
                send_x(4)
            relay_a(s)
        with jax.named_scope(f"a_norm{s}"):
            layer_norm(s)
        with jax.named_scope(f"a_wait_d{s}"):
            wait(w1s.at[pl.ds(0, 2)], recv_sem.at[A_D2D + s])
        with jax.named_scope(f"a_tiles{s}"):
            def a_tile(t, _):
                q = t // (s + 1)
                g, j = t - q * (t - s), s - q * (t - s)
                p = col * 8 + 2 * j
                for k in (0, 256):
                    unit(pl.multiple_of(g * 512 + k, 256), 256, (p, p + 1))
                finish()
                return 0

            lax.fori_loop(0, 2 * s + 1, a_tile, 0)

    early = X_ROWS[4][0]
    third = early // 3
    with jax.named_scope("a_norm3"):
        layer_norm(3)
    quarter = early // 4

    def first(e):
        with jax.named_scope(f"first{e}"):
            unit(*X_ROWS[3], pieces(col, 2 * e, 2 * e + 2))

    def a_unit(q):
        unit(q * quarter, quarter, pieces(col, 6, 8))

    def b_unit(e, q):
        unit(q * quarter, quarter, pieces(other, e, e + 1))

    def by(e, h):
        with jax.named_scope(f"by{e}{h}"):
            relay_by(e, h)

    def bx(e):
        with jax.named_scope(f"bx{e}"):
            relay_bx(e)

    def b_arrived(e):
        with jax.named_scope(f"bd{e}"):
            wait(w2s.at[0], recv_sem.at[B_D2D + e])

    first(0)
    by(0, 0)
    first(1)
    first(2)
    by(0, 1)
    with jax.named_scope("a3"):
        relay_a(3)
    by(1, 0)
    with jax.named_scope("ad3"):
        wait(w1s.at[pl.ds(0, 2)], recv_sem.at[A_D2D + 3])
    a_unit(0)
    by(1, 1)
    a_unit(1)
    a_unit(2)
    bx(0)
    by(2, 0)
    a_unit(3)
    for e in range(5):
        by(e + 2, 1)
        b_arrived(e)
        b_unit(e, 0)
        b_unit(e, 1)
        bx(e + 1)
        by(e + 3, 0)
        b_unit(e, 2)
        b_unit(e, 3)
    by(7, 1)
    b_arrived(5)
    b_unit(5, 0)
    b_unit(5, 1)
    bx(6)
    b_unit(5, 2)
    b_unit(5, 3)
    b_arrived(6)
    for q in range(4):
        b_unit(6, q)
    finish()
    bx(7)
    with jax.named_scope("c_norm"):
        layer_norm(4)
    with jax.named_scope("c_tiles"):
        last = pieces(col, 0, 8) + pieces(other, 0, 7)
        for ps in (last[:8], last[8:]):
            @pl.when(row >= 0)
            def _():
                unit(early, tokens - early, ps)
                finish()
    b_arrived(7)
    with jax.named_scope("d_tile"):
        def write(rows, value):
            ys[rows, :] = value.astype(jnp.bfloat16)

        for q in range(4):
            unit(q * (tokens // 4), tokens // 4, pieces(other, 7, 8), write)
        finish()

    with jax.named_scope("sent"):
        wait(w1s.at[pl.ds(0, 14)], send_sem.at[S_W1])
        wait(w2s.at[pl.ds(0, 12)], send_sem.at[S_W2])
        wait(xs.at[0], send_sem.at[S_X])
        wait(gs.at[0], send_sem.at[S_G])


def solution(mesh):
    act_spec = P(None, ("dp", "row"), "col")

    def per_device(x_blk, gamma_blk, w_in_blk, w_out_blk):
        feats = x_blk.shape[2]
        tokens = x_blk.shape[0] * x_blk.shape[1]
        d_model = 2 * feats
        n_pieces = 2 * w_in_blk.shape[1] // PC
        ins = (x_blk.reshape(tokens, feats), gamma_blk.reshape(1, feats), w_in_blk, w_out_blk)
        y = pl.pallas_call(
            kernel,
            name="mlp",
            out_shape=jax.ShapeDtypeStruct((tokens, feats), jnp.bfloat16),
            in_specs=[pl.BlockSpec(memory_space=pltpu.HBM)] * 4,
            out_specs=pl.BlockSpec(memory_space=pltpu.VMEM),
            scratch_shapes=[
                pltpu.VMEM((2, tokens, feats), jnp.bfloat16),
                pltpu.VMEM((n_pieces, d_model, PC), jnp.bfloat16),
                pltpu.VMEM((n_pieces, PC, feats), jnp.bfloat16),
                pltpu.VMEM((tokens, d_model), jnp.bfloat16),
                pltpu.VMEM((tokens, feats), jnp.float32),
                pltpu.VMEM((2, 1, feats), jnp.float32),
                pltpu.SemaphoreType.DMA((4,)),
                pltpu.SemaphoreType.DMA((4,)),
                pltpu.SemaphoreType.DMA((N_RECV,)),
            ],
            compiler_params=pltpu.CompilerParams(collective_id=0, has_side_effects=True, vmem_limit_bytes=52000000),
        )(*[pltpu.with_memory_space_constraint(a, pltpu.HBM) for a in ins])
        return y.reshape(x_blk.shape)

    return jax.shard_map(per_device, mesh=mesh, in_specs=(act_spec, P("col"), P("row", "col"), P("row", "col")), out_specs=act_spec, check_vma=False)
```
